256 devices in a mesh: cell: 64 (over x, z, y_hi), gene: 4 (over y_lo, core).
Axes of the slice: x: 4, y: 4 (y_hi: 2, y_lo: 2; y = y_hi * 2 + y_lo), z: 8, core: 2. Of those that a mesh axis runs over, the one named last changes fastest.
Arguments:
- counts: int32 [16384, 4096], P('cell', 'gene'), may hold values from 0 to 7
- totals: int32 [16384], P('cell'), may hold values from 1000 to 19999
- cell_factors: float32 [16384, 32], P('cell'), may hold values from -0.9 to 0.9
- gene_loadings: float32 [4096, 32], P('gene'), may hold values from -0.9 to 0.9
Outputs:
- new_factors: float32 [16384, 32], P('cell')
- new_loadings: float32 [4096, 32], P('gene')
- deviance: float32 [4096], P('gene')
The draws below stay inside these ranges and needn't reach their ends.
All inputs are finite; a program needn't handle non-finite values.
Results may differ from the reference program's by a relative error of at most 0.0044.
Values sent between devices are 32-bit elements; how exact they have to be, the bound alone decides.
A program may use at most 128 MiB of HBM per device.

```python
import math
import jax
import jax.numpy as jnp
from jax import lax

L = 32
GENES = 4096
CD = 256
CELLS = 16384
N_CELL = 64


def set_ends(result, rng, smallest, largest):
    shape = result.shape
    place = [jax.random.randint(jax.random.fold_in(rng, axis), (), 0, shape[axis]) for axis in range(len(shape))]
    result = result.at[tuple(place)].set(smallest)
    longest = shape.index(max(shape))
    place[longest] = (place[longest] + 1) % shape[longest]
    return result.at[tuple(place)].set(largest)


def block_levels(stream_key, shape, shards, smallest, top_value):
    gain = 1.0
    for dim, parts in shards:
        draws = jax.random.uniform(jax.random.fold_in(jax.random.fold_in(stream_key, 6), dim), (parts,), jnp.float32, smallest / len(shards), top_value / len(shards))
        gain = gain * jnp.repeat(jnp.exp(draws), shape[dim] // parts).reshape((-1,) + (1,) * (len(shape) - 1 - dim))
    return gain


def gaussian(rng, extent, deviation, bound, shards=(), dtype=jnp.bfloat16):
    result = deviation * jax.random.normal(rng, extent, jnp.float32)
    if shards:
        result = result * block_levels(rng, extent, shards, -0.22, 0.18)
    return jnp.clip(result, -bound, bound).astype(dtype)


def setup_inputs(seed: int = 0) -> dict:
    keys = jax.random.split(jax.random.key(seed), 5)
    counts = set_ends(jax.random.randint(keys[0], (CELLS, GENES), 0, 8), jax.random.fold_in(keys[0], 1), 0, 7).astype(jnp.int32)
    totals = set_ends(jax.random.randint(keys[1], (CELLS,), 1000, 20000), jax.random.fold_in(keys[1], 1), 1000, 19999).astype(jnp.int32)
    cell_factors = gaussian(keys[2], (CELLS, L), 0.15, 0.9, ((0, 64),), jnp.float32)
    gene_loadings = gaussian(keys[3], (GENES, L), 0.15, 0.9, ((0, 4),), jnp.float32)
    return {"counts": counts, "totals": totals, "cell_factors": cell_factors, "gene_loadings": gene_loadings}


RIDGE = 1.0
DAMPING = 0.1
SCALE_TOTAL = 5000.0

def outer_table(factors):
    width = factors.shape[1]
    product = factors[:, :, None] * factors[:, None, :]
    return product.reshape(factors.shape[0], width * width).astype(jnp.bfloat16)

def newton_solve(curvature, gradient):
    width = gradient.shape[1]
    matrix = jnp.transpose(curvature.reshape(gradient.shape[0], width, width), (1, 2, 0))
    diagonal_mean = sum((matrix[index, index] for index in range(width))) / width
    shift = RIDGE + DAMPING * diagonal_mean
    right = jnp.transpose(gradient)
    columns = []
    for column in range(width):
        current = matrix[:, column]
        if column > 0:
            stacked = jnp.stack(columns)
            current = current - lax.optimization_barrier(jnp.sum(stacked * stacked[:, column][:, None, :], axis=0))
        current = current + jnp.where(jnp.arange(width) == column, 1.0, 0.0).astype(jnp.float32)[:, None] * shift[None, :]
        pivot = jnp.sqrt(current[column])
        mask = (jnp.arange(width) >= column).astype(jnp.float32)[:, None]
        columns.append(mask * current / pivot[None, :])
    lower = jnp.stack(columns, axis=1)
    forward = []
    for row in range(width):
        value = right[row]
        for inner in range(row):
            value = value - lower[row, inner] * forward[inner]
        forward.append(value / lower[row, row])
    backward = [None] * width
    for row in range(width - 1, -1, -1):
        value = forward[row]
        for inner in range(row + 1, width):
            value = value - lower[inner, row] * backward[inner]
        backward[row] = value / lower[row, row]
    return jnp.transpose(jnp.stack(backward))

def predict(offset, factors, loadings):
    linear = offset[:, None] + jnp.dot(factors, loadings.T, precision=lax.Precision.HIGHEST)
    return (linear, jnp.exp(linear))

def gene_contract(counts, expected, loadings):
    weights = expected.astype(jnp.bfloat16)
    residual = (counts.astype(jnp.float32) - expected).astype(jnp.bfloat16)
    gradient = jnp.dot(residual, loadings.astype(jnp.bfloat16), preferred_element_type=jnp.float32)
    curvature = jnp.dot(weights, outer_table(loadings), preferred_element_type=jnp.float32)
    return (gradient, curvature)

def cell_contract(counts, linear, expected, factors):
    counts_real = counts.astype(jnp.float32)
    weights = expected.astype(jnp.bfloat16)
    residual = (counts_real - expected).astype(jnp.bfloat16)
    dims = (((0,), (0,)), ((), ()))
    gradient = lax.dot_general(residual, factors.astype(jnp.bfloat16), dims, preferred_element_type=jnp.float32)
    curvature = lax.dot_general(weights, outer_table(factors), dims, preferred_element_type=jnp.float32)
    terms = 2.0 * (counts_real * (jnp.log(jnp.maximum(counts_real, 1.0)) - linear) - counts_real + expected)
    return (gradient, curvature, lax.optimization_barrier(jnp.sum(terms, axis=0)))

def reference(counts, totals, cell_factors, gene_loadings):
    offset = jnp.log(totals.astype(jnp.float32)) - math.log(SCALE_TOTAL)
    count_blocks = counts.reshape(N_CELL, CD, GENES)
    offset_blocks = offset.reshape(N_CELL, CD)
    factor_blocks = cell_factors.reshape(N_CELL, CD, L)

    def factor_update(block):
        count_block, offset_block, factor_block = block
        linear, expected = predict(offset_block, factor_block, gene_loadings)
        gradient, curvature = gene_contract(count_block, expected, gene_loadings)
        return factor_block + newton_solve(curvature, gradient - RIDGE * factor_block)
    new_blocks = lax.map(factor_update, (count_blocks, offset_blocks, factor_blocks))
    new_factors = new_blocks.reshape(CELLS, L)

    def loading_update(running, block):
        count_block, offset_block, factor_block = block
        linear, expected = predict(offset_block, factor_block, gene_loadings)
        gradient, curvature, deviance_part = cell_contract(count_block, linear, expected, factor_block)
        return ((running[0] + gradient, running[1] + curvature, running[2] + deviance_part), None)
    initial = (jnp.zeros((GENES, L), jnp.float32), jnp.zeros((GENES, L * L), jnp.float32), jnp.zeros((GENES,), jnp.float32))
    totals_sum, unused = lax.scan(loading_update, initial, (count_blocks, offset_blocks, new_blocks))
    gradient_sum, curvature_sum, deviance_sum = totals_sum
    new_loadings = gene_loadings + newton_solve(curvature_sum, gradient_sum - RIDGE * gene_loadings)
    deviance = deviance_sum / CELLS
    return (new_factors, new_loadings, deviance)
```

```python
import math

import jax
import jax.numpy as jnp
from jax import lax
from jax.experimental import pallas as pl
from jax.experimental.pallas import tpu as pltpu
from jax.sharding import PartitionSpec as P

F32, BF16 = jnp.float32, jnp.bfloat16
MESH = pl.DeviceIdType.MESH

RIDGE = 1.0
DAMPING = 0.1
LOG_SCALE = math.log(5000.0)

WIDTH = 32
X, Z, YH = 4, 8, 2
CELL_DEVICES = X * Z * YH
T = X * YH
CELLS = 256
GENES = 1024
LANES = 128
GENES_Z = GENES // Z
OWN_GENES = GENES_Z // T
HALF = LANES // 2

HEIGHT = [WIDTH - c // 8 * 8 for c in range(WIDTH)]
START = [sum(HEIGHT[:c]) for c in range(WIDTH)]
TRIANGLE = sum(HEIGHT)
ROWS1 = TRIANGLE + WIDTH
ROWS2 = 704
PIECE2 = ROWS2 // T


def parts_of(value):
    high = value.astype(BF16).astype(F32)
    rest = value - high
    middle = rest.astype(BF16).astype(F32)
    return high, middle, rest - middle


def left_stack(factors, offset):
    high, middle, low = parts_of(factors)
    row = lax.broadcasted_iota(jnp.int32, (16, factors.shape[1]), 0)
    off_high, off_middle, off_low = parts_of(offset)
    extra = jnp.where(
        row == 0, off_high, jnp.where(row == 1, off_middle, jnp.where(row == 2, off_low, 0.0))
    )
    return jnp.concatenate([high, high, middle, middle, high, low, extra], axis=0).astype(BF16)


def right_stack(loadings):
    high, middle, low = parts_of(loadings)
    extra = jnp.ones((16, loadings.shape[1]), F32)
    return jnp.concatenate([high, middle, high, middle, low, high, extra], axis=0).astype(BF16)


def predict(left, right):
    return lax.dot_general(left, right, (((0,), (0,)), ((), ())), preferred_element_type=F32)


def write_table(table_ref, columns, rows):
    for c in range(0, WIDTH, 2):
        first = c // 8 * 8
        pair = jnp.concatenate(
            [rows[first:] * rows[c : c + 1], rows[first:] * rows[c + 1 : c + 2]], axis=0
        )
        table_ref[START[c] : START[c] + 2 * HEIGHT[c], columns] = pair.astype(BF16)
    table_ref[TRIANGLE : TRIANGLE + WIDTH, columns] = rows.astype(BF16)


def solve(matrix_ref, right_ref, column_ref, inverse_ref):
    for j in range(8, WIDTH):
        for block in range(j // 8):
            matrix_ref[WIDTH * j + 8 * block : WIDTH * j + 8 * block + 8, :] = matrix_ref[
                pl.ds(WIDTH * 8 * block + j, 8, stride=WIDTH), :
            ]
    diagonal = matrix_ref[pl.ds(0, WIDTH, stride=WIDTH + 1), :]
    shift = RIDGE + DAMPING * (jnp.sum(diagonal, axis=0, keepdims=True) / WIDTH)
    matrix_ref[pl.ds(0, WIDTH, stride=WIDTH + 1), :] = diagonal + shift
    row = lax.broadcasted_iota(jnp.int32, (WIDTH, LANES), 0)
    for group in range(WIDTH // 8):

        def step(c, carry):
            column = matrix_ref[pl.ds(pl.multiple_of(c * WIDTH, WIDTH), WIDTH), :]
            column_ref[...] = column
            inverse = 1.0 / column_ref[pl.ds(c, 1), :]
            inverse_ref[pl.ds(c, 1), :] = inverse
            scaled = jnp.where(row == c, 0.0, column * inverse)
            right_ref[...] = right_ref[...] - scaled * right_ref[pl.ds(c, 1), :]
            for j in range(8 * group, WIDTH):
                at = slice(WIDTH * j, WIDTH * j + WIDTH)
                matrix_ref[at, :] = matrix_ref[at, :] - scaled * column_ref[j : j + 1, :]
            return carry

        lax.fori_loop(8 * group, 8 * group + 8, step, 0)
    return right_ref[...] * inverse_ref[...]


def load_matrix(matrix_ref, packed_ref):
    for c in range(WIDTH):
        first = WIDTH - HEIGHT[c]
        matrix_ref[WIDTH * c + first : WIDTH * c + WIDTH, :] = packed_ref[
            START[c] : START[c] + HEIGHT[c], :
        ]


def kernel(
    counts_ref, totals_ref, factors_ref, loadings_ref,
    new_factors_ref, new_loadings_ref, deviance_ref,
    loadings_t, factors_t, table1, weights1, residual1, sums1, core_in, yl_out, yl_in,
    packed, matrix, right, column, inverse,
    counts_z, totals_z, factor_slots, table2, both2, sums2, piece_out, piece_in, final_out,
    final_in, final_t,
    counts_send, counts_recv, totals_send, totals_recv, pair_send, pair_recv,
    factor_send, factor_recv, piece_send, piece_recv, final_send, final_recv,
):
    cell = lax.axis_index("cell")
    gene = lax.axis_index("gene")
    x, z, yh = cell // (Z * YH), (cell // YH) % Z, cell % YH
    yl, core = gene // 2, gene % 2
    t = x * YH + yh
    quarter = core * 2 + yl

    def cell_at(x_, z_, yh_):
        return (x_ * Z + z_) * YH + yh_

    barrier = pltpu.get_barrier_semaphore()

    def greet_cell(d, carry):
        pl.semaphore_signal(
            barrier, inc=1, device_id={"cell": (cell + d) % CELL_DEVICES, "gene": gene},
            device_id_type=MESH,
        )
        return carry

    def greet_gene(k, carry):
        pl.semaphore_signal(
            barrier, inc=1,
            device_id={"cell": cell_at(x, k // 3, yh), "gene": (gene + 1 + k % 3) % 4},
            device_id_type=MESH,
        )
        return carry

    lax.fori_loop(1, CELL_DEVICES, greet_cell, 0)
    lax.fori_loop(0, 3 * Z, greet_gene, 0)
    pl.semaphore_wait(barrier, CELL_DEVICES - 1 + 3 * Z)

    def counts_copy(d):
        other = (z + d) % Z
        return pltpu.make_async_remote_copy(
            src_ref=counts_ref.at[:, pl.ds(pl.multiple_of(other * GENES_Z, GENES_Z), GENES_Z)],
            dst_ref=counts_z.at[z],
            send_sem=counts_send.at[d], recv_sem=counts_recv.at[z],
            device_id={"cell": cell_at(x, other, yh), "gene": gene}, device_id_type=MESH,
        )

    def totals_copy(d):
        other = (z + d) % Z
        return pltpu.make_async_remote_copy(
            src_ref=totals_ref, dst_ref=totals_z.at[z],
            send_sem=totals_send.at[d], recv_sem=totals_recv.at[z],
            device_id={"cell": cell_at(x, other, yh), "gene": gene}, device_id_type=MESH,
        )

    def counts_arrived(d):
        other = (z + d) % Z
        return pltpu.make_async_remote_copy(
            src_ref=counts_z.at[other], dst_ref=counts_z.at[other],
            send_sem=counts_send.at[d], recv_sem=counts_recv.at[other],
            device_id={"cell": cell_at(x, other, yh), "gene": gene}, device_id_type=MESH,
        )

    def totals_arrived(d):
        other = (z + d) % Z
        return pltpu.make_async_remote_copy(
            src_ref=totals_z.at[other], dst_ref=totals_z.at[other],
            send_sem=totals_send.at[d], recv_sem=totals_recv.at[other],
            device_id={"cell": cell_at(x, other, yh), "gene": gene}, device_id_type=MESH,
        )

    for d in range(1, Z):
        totals_copy(d).start()
    for d in range(1, Z):
        counts_copy(d).start()
    counts_z[z] = counts_ref[:, pl.ds(pl.multiple_of(z * GENES_Z, GENES_Z), GENES_Z)]
    totals_z[z] = totals_ref[...]

    lane = lax.broadcasted_iota(jnp.int32, (1, LANES), 1)

    def offset_of(slot):
        logs = jnp.log(totals_z[slot].astype(F32)) - LOG_SCALE
        return jnp.concatenate([logs[0:1], logs[1:2]], axis=1)

    loadings = loadings_ref[...].T
    for k in range(Z):
        loadings_t[k] = loadings[:, k * LANES : (k + 1) * LANES]
    factors = factors_ref[...].T
    factors_t[0] = factors[:, :LANES]
    factors_t[1] = factors[:, LANES:]
    left = left_stack(factors, offset_of(z))
    for k in range(Z):
        columns = slice(k * LANES, (k + 1) * LANES)
        rows = loadings_t[k]
        write_table(table1, columns, rows)
        expected = jnp.exp(predict(left, right_stack(rows)))
        weights1[:, columns] = expected.astype(BF16)
        residual1[:, columns] = (counts_ref[:, columns].astype(F32) - expected).astype(BF16)
    dims = (((1,), (1,)), ((), ()))
    curvature = lax.dot_general(
        table1[:TRIANGLE, :], weights1[...], dims, preferred_element_type=F32
    )
    gradient = lax.dot_general(
        table1[TRIANGLE:, :], residual1[...], dims, preferred_element_type=F32
    )
    for half in range(2):
        columns = slice(half * LANES, (half + 1) * LANES)
        sums1[half, :TRIANGLE, :] = curvature[:, columns]
        sums1[half, TRIANGLE:, :] = gradient[:, columns]

    core_copy = pltpu.make_async_remote_copy(
        src_ref=sums1.at[1 - core], dst_ref=core_in,
        send_sem=pair_send.at[0], recv_sem=pair_recv.at[0],
        device_id={"cell": cell, "gene": yl * 2 + 1 - core}, device_id_type=MESH,
    )
    core_copy.start()
    core_copy.wait_recv()
    middle = ROWS1 // 2
    top = sums1[core, :middle, :] + core_in[:middle, :]
    bottom = sums1[core, middle:, :] + core_in[middle:, :]
    low = lane < HALF
    first_pack = jnp.where(low, top, pltpu.roll(bottom, HALF, 1))
    second_pack = jnp.where(low, pltpu.roll(top, HALF, 1), bottom)
    yl_out[...] = jnp.where(yl == 0, second_pack, first_pack)
    yl_copy = pltpu.make_async_remote_copy(
        src_ref=yl_out, dst_ref=yl_in,
        send_sem=pair_send.at[1], recv_sem=pair_recv.at[1],
        device_id={"cell": cell, "gene": (1 - yl) * 2 + core}, device_id_type=MESH,
    )
    yl_copy.start()
    own_pack = jnp.where(yl == 0, first_pack, second_pack)
    yl_copy.wait_recv()
    total = own_pack + yl_in[...]
    packed[:middle, :] = total
    packed[middle:ROWS1, :] = pltpu.roll(total, HALF, 1)
    load_matrix(matrix, packed)
    old = factors_t[core]
    old = jnp.where(yl == 0, old, pltpu.roll(old, HALF, 1))
    right[...] = packed[TRIANGLE:ROWS1, :] - RIDGE * old
    new = old + solve(matrix, right, column, inverse)
    factor_slots[z, quarter] = jnp.where(low, new[:16], pltpu.roll(new[16:], HALF, 1))

    def factor_copy(k):
        other, step = k // 4, k % 4
        target = (z + other) % Z
        return pltpu.make_async_remote_copy(
            src_ref=factor_slots.at[z, quarter], dst_ref=factor_slots.at[z, quarter],
            send_sem=factor_send.at[k], recv_sem=factor_recv.at[z * 4 + quarter],
            device_id={"cell": cell_at(x, target, yh), "gene": (gene + step) % 4},
            device_id_type=MESH,
        )

    def factor_arrived(k):
        other, step = k // 4, k % 4
        source_z, source_gene = (z + other) % Z, (gene + step) % 4
        source_quarter = source_gene % 2 * 2 + source_gene // 2
        slot = factor_slots.at[source_z, source_quarter]
        return pltpu.make_async_remote_copy(
            src_ref=slot, dst_ref=slot,
            send_sem=factor_send.at[k], recv_sem=factor_recv.at[source_z * 4 + source_quarter],
            device_id={"cell": cell_at(x, source_z, yh), "gene": source_gene},
            device_id_type=MESH,
        )

    def run(action, first, last):
        def body(k, carry):
            action(k)
            return carry

        lax.fori_loop(first, last, body, 0)

    run(lambda k: factor_copy(k).start(), 1, 4 * Z)
    run(lambda k: factor_arrived(k).wait_recv(), 1, 4 * Z)
    for d in range(1, Z):
        totals_arrived(d).wait_recv()
    for d in range(1, Z):
        counts_arrived(d).wait_recv()

    def tile_of(slot, pair):
        first, second = factor_slots[slot, 2 * pair], factor_slots[slot, 2 * pair + 1]
        return jnp.concatenate(
            [
                jnp.where(low, first, pltpu.roll(second, HALF, 1)),
                jnp.where(low, pltpu.roll(first, HALF, 1), second),
            ],
            axis=0,
        )

    new_factors_ref[:LANES, :] = tile_of(z, 0).T
    new_factors_ref[LANES:, :] = tile_of(z, 1).T

    right2 = right_stack(loadings_t[z])
    deviance = jnp.zeros((8, LANES), F32)
    for k in range(Z):
        rows = jnp.concatenate([tile_of(k, 0), tile_of(k, 1)], axis=1)
        columns = slice(k * CELLS, (k + 1) * CELLS)
        write_table(table2, columns, rows)
        linear = predict(left_stack(rows, offset_of(k)), right2)
        expected = jnp.exp(linear)
        counts = counts_z[k].astype(F32)
        both2[columns, :LANES] = expected.astype(BF16)
        both2[columns, LANES:] = (counts - expected).astype(BF16)
        terms = 2.0 * (counts * (jnp.log(jnp.maximum(counts, 1.0)) - linear) - counts + expected)
        deviance = deviance + jnp.sum(terms.reshape(CELLS // 8, 8, LANES), axis=0)
    products = jnp.dot(table2[...], both2[...], preferred_element_type=F32)
    sums2[:TRIANGLE, :] = products[:TRIANGLE, :LANES]
    sums2[TRIANGLE:ROWS1, :] = products[TRIANGLE:, LANES:]
    sums2[ROWS1 : ROWS1 + 8, :] = deviance
    sums2[ROWS1 + 8 :, :] = jnp.zeros((ROWS2 - ROWS1 - 8, LANES), F32)

    block = lane // OWN_GENES
    for target in range(T):
        piece = jnp.zeros((PIECE2, LANES), F32)
        for k in range(T):
            rows = sums2[k * PIECE2 : (k + 1) * PIECE2, :]
            moved = rows if k == target else pltpu.roll(rows, (k - target) * OWN_GENES % LANES, 1)
            piece = jnp.where(block == k, moved, piece)
        piece_out[target] = piece

    def piece_copy(d):
        target = (t + d) % T
        return pltpu.make_async_remote_copy(
            src_ref=piece_out.at[target], dst_ref=piece_in.at[t],
            send_sem=piece_send.at[d], recv_sem=piece_recv.at[t],
            device_id={"cell": cell_at(target // YH, z, target % YH), "gene": gene},
            device_id_type=MESH,
        )

    def piece_arrived(d):
        source = (t + d) % T
        return pltpu.make_async_remote_copy(
            src_ref=piece_in.at[source], dst_ref=piece_in.at[source],
            send_sem=piece_send.at[d], recv_sem=piece_recv.at[source],
            device_id={"cell": cell_at(source // YH, z, source % YH), "gene": gene},
            device_id_type=MESH,
        )

    for d in range(1, T):
        piece_copy(d).start()
    piece_in[t] = piece_out[t]
    for d in range(1, T):
        piece_arrived(d).wait_recv()
    total = piece_in[0]
    for k in range(1, T):
        total = total + piece_in[k]
    for k in range(T):
        packed[k * PIECE2 : (k + 1) * PIECE2, :] = (
            total if k == 0 else pltpu.roll(total, LANES - k * OWN_GENES, 1)
        )
    load_matrix(matrix, packed)
    old = loadings_t[z]
    own = old
    for k in range(1, T):
        own = jnp.where(t == k, pltpu.roll(old, LANES - k * OWN_GENES, 1), own)
    right[...] = packed[TRIANGLE:ROWS1, :] - RIDGE * own
    new = own + solve(matrix, right, column, inverse)
    mean = jnp.sum(packed[ROWS1 : ROWS1 + 8, :], axis=0, keepdims=True) / (CELLS * CELL_DEVICES)
    message = jnp.where(block == 0, new[:8], 0.0)
    for k in range(1, 4):
        message = jnp.where(
            block == k, pltpu.roll(new[8 * k : 8 * k + 8], k * OWN_GENES, 1), message
        )
    mean = jnp.broadcast_to(mean, (8, LANES))
    final_out[...] = jnp.where(block == 4, pltpu.roll(mean, 4 * OWN_GENES, 1), message)

    def final_copy(d):
        return pltpu.make_async_remote_copy(
            src_ref=final_out, dst_ref=final_in.at[t, z],
            send_sem=final_send.at[d], recv_sem=final_recv.at[cell],
            device_id={"cell": (cell + d) % CELL_DEVICES, "gene": gene}, device_id_type=MESH,
        )

    def final_arrived(d):
        source = (cell + d) % CELL_DEVICES
        source_x, source_z, source_yh = source // (Z * YH), (source // YH) % Z, source % YH
        slot = final_in.at[source_x * YH + source_yh, source_z]
        return pltpu.make_async_remote_copy(
            src_ref=slot, dst_ref=slot,
            send_sem=final_send.at[d], recv_sem=final_recv.at[source],
            device_id={"cell": source, "gene": gene}, device_id_type=MESH,
        )

    run(lambda d: final_copy(d).start(), 1, CELL_DEVICES)
    final_in[t, z] = final_out[...]
    run(lambda d: final_arrived(d).wait_recv(), 1, CELL_DEVICES)
    for j in range(5):
        value = jnp.zeros((8 * Z, LANES), F32)
        for k in range(T):
            rows = final_in[k].reshape(8 * Z, LANES)
            moved = rows if k == j else pltpu.roll(rows, (k - j) * OWN_GENES % LANES, 1)
            value = jnp.where(block == k, moved, value)
        final_t[j] = value
    for k in range(Z):
        eight = slice(8 * k, 8 * k + 8)
        tile = jnp.concatenate([final_t[j, eight, :] for j in range(4)], axis=0)
        new_loadings_ref[k * LANES : (k + 1) * LANES, :] = tile.T
        deviance_ref[k : k + 1, :] = final_t[4, 8 * k : 8 * k + 1, :]

    for d in range(1, Z):
        counts_copy(d).wait_send()
        totals_copy(d).wait_send()
    core_copy.wait_send()
    yl_copy.wait_send()
    run(lambda k: factor_copy(k).wait_send(), 1, 4 * Z)
    for d in range(1, T):
        piece_copy(d).wait_send()
    run(lambda d: final_copy(d).wait_send(), 1, CELL_DEVICES)


def on_device(counts, totals, cell_factors, gene_loadings):
    vmem = pl.BlockSpec(memory_space=pltpu.VMEM)
    dma = pltpu.SemaphoreType.DMA
    new_factors, new_loadings, deviance = pl.pallas_call(
        kernel,
        out_shape=(
            jax.ShapeDtypeStruct((CELLS, WIDTH), F32),
            jax.ShapeDtypeStruct((GENES, WIDTH), F32),
            jax.ShapeDtypeStruct((Z, LANES), F32),
        ),
        in_specs=[vmem] * 4,
        out_specs=(vmem,) * 3,
        scratch_shapes=[
            pltpu.VMEM((Z, WIDTH, LANES), F32),
            pltpu.VMEM((2, WIDTH, LANES), F32),
            pltpu.VMEM((ROWS1, GENES), BF16),
            pltpu.VMEM((CELLS, GENES), BF16),
            pltpu.VMEM((CELLS, GENES), BF16),
            pltpu.VMEM((2, ROWS1, LANES), F32),
            pltpu.VMEM((ROWS1, LANES), F32),
            pltpu.VMEM((ROWS1 // 2, LANES), F32),
            pltpu.VMEM((ROWS1 // 2, LANES), F32),
            pltpu.VMEM((ROWS2, LANES), F32),
            pltpu.VMEM((WIDTH * WIDTH, LANES), F32),
            pltpu.VMEM((WIDTH, LANES), F32),
            pltpu.VMEM((WIDTH, LANES), F32),
            pltpu.VMEM((WIDTH, LANES), F32),
            pltpu.VMEM((Z, CELLS, LANES), jnp.int32),
            pltpu.VMEM((Z, 2, LANES), jnp.int32),
            pltpu.VMEM((Z, 4, 16, LANES), F32),
            pltpu.VMEM((ROWS1, Z * CELLS), BF16),
            pltpu.VMEM((Z * CELLS, 2 * LANES), BF16),
            pltpu.VMEM((ROWS2, LANES), F32),
            pltpu.VMEM((T, PIECE2, LANES), F32),
            pltpu.VMEM((T, PIECE2, LANES), F32),
            pltpu.VMEM((8, LANES), F32),
            pltpu.VMEM((T, Z, 8, LANES), F32),
            pltpu.VMEM((5, 8 * Z, LANES), F32),
            dma((Z,)), dma((Z,)), dma((Z,)), dma((Z,)), dma((2,)), dma((2,)),
            dma((4 * Z,)), dma((4 * Z,)), dma((T,)), dma((T,)),
            dma((CELL_DEVICES,)), dma((CELL_DEVICES,)),
        ],
        compiler_params=pltpu.CompilerParams(
            collective_id=0, has_side_effects=True, vmem_limit_bytes=48 * 1024 * 1024
        ),
        name="sweep",
    )(counts, totals.reshape(2, LANES), cell_factors, gene_loadings)
    return new_factors, new_loadings, deviance.reshape(GENES)


def solution(mesh):
    return jax.shard_map(
        on_device,
        mesh=mesh,
        in_specs=(P("cell", "gene"), P("cell"), P("cell", None), P("gene", None)),
        out_specs=(P("cell", None), P("gene", None), P("gene")),
        check_vma=False,
    )
```

```python
import math

import jax
import jax.numpy as jnp
from jax import lax
from jax.experimental import pallas as pl
from jax.experimental.pallas import tpu as pltpu
from jax.sharding import PartitionSpec as P

F32, BF16 = jnp.float32, jnp.bfloat16
MESH = pl.DeviceIdType.MESH

RIDGE = 1.0
DAMPING = 0.1
LOG_SCALE = math.log(5000.0)

WIDTH = 32
X, Z, YH = 4, 8, 2
CELL_DEVICES = X * Z * YH
T = X * YH
CELLS = 256
GENES = 1024
LANES = 128
GENES_Z = GENES // Z
OWN_GENES = GENES_Z // T
HALF = LANES // 2
CHUNK = 256
ORDER = (0, 1, 7, 2, 6, 3, 5, 4)

HEIGHT = [WIDTH - c // 8 * 8 for c in range(WIDTH)]
START = [sum(HEIGHT[:c]) for c in range(WIDTH)]
TRIANGLE = sum(HEIGHT)
ROWS1 = TRIANGLE + WIDTH
LOCAL = WIDTH + 8
ROWS2 = 704
PIECE2 = ROWS2 // T
MESSAGE = 5


def parts_of(value):
    high = value.astype(BF16).astype(F32)
    rest = value - high
    middle = rest.astype(BF16).astype(F32)
    return high, middle, rest - middle


def left_stack(factors, offset):
    high, middle, low = parts_of(factors)
    row = lax.broadcasted_iota(jnp.int32, (16, factors.shape[1]), 0)
    off_high, off_middle, off_low = parts_of(offset)
    extra = jnp.where(
        row == 0, off_high, jnp.where(row == 1, off_middle, jnp.where(row == 2, off_low, 0.0))
    )
    return jnp.concatenate([high, high, middle, middle, high, low, extra], axis=0).astype(BF16)


def right_stack(loadings):
    high, middle, low = parts_of(loadings)
    extra = jnp.ones((16, loadings.shape[1]), F32)
    return jnp.concatenate([high, middle, high, middle, low, high, extra], axis=0).astype(BF16)


def predict(left, right):
    return lax.dot_general(left, right, (((0,), (0,)), ((), ())), preferred_element_type=F32)


def write_table(table_ref, columns, rows):
    for c in range(0, WIDTH, 2):
        first = c // 8 * 8
        pair = jnp.concatenate(
            [rows[first:] * rows[c : c + 1], rows[first:] * rows[c + 1 : c + 2]], axis=0
        )
        table_ref[START[c] : START[c] + 2 * HEIGHT[c], columns] = pair.astype(BF16)
    table_ref[TRIANGLE : TRIANGLE + WIDTH, columns] = rows.astype(BF16)


def solve(matrix_ref, right_ref, column_ref, inverse_ref):
    for j in range(8, WIDTH):
        for block in range(j // 8):
            matrix_ref[WIDTH * j + 8 * block : WIDTH * j + 8 * block + 8, :] = matrix_ref[
                pl.ds(WIDTH * 8 * block + j, 8, stride=WIDTH), :
            ]
    diagonal = matrix_ref[pl.ds(0, WIDTH, stride=WIDTH + 1), :]
    shift = RIDGE + DAMPING * (jnp.sum(diagonal, axis=0, keepdims=True) / WIDTH)
    matrix_ref[pl.ds(0, WIDTH, stride=WIDTH + 1), :] = diagonal + shift
    row = lax.broadcasted_iota(jnp.int32, (WIDTH, LANES), 0)
    for group in range(WIDTH // 8):

        def step(c, carry):
            column = matrix_ref[pl.ds(pl.multiple_of(c * WIDTH, WIDTH), WIDTH), :]
            column_ref[...] = column
            inverse = 1.0 / column_ref[pl.ds(c, 1), :]
            inverse_ref[pl.ds(c, 1), :] = inverse
            scaled = jnp.where(row == c, 0.0, column * inverse)
            right_ref[...] = right_ref[...] - scaled * right_ref[pl.ds(c, 1), :]
            for j in range(8 * group, WIDTH):
                at = slice(WIDTH * j, WIDTH * j + WIDTH)
                matrix_ref[at, :] = matrix_ref[at, :] - scaled * column_ref[j : j + 1, :]
            return carry

        lax.fori_loop(8 * group, 8 * group + 8, step, 0)
    return right_ref[...] * inverse_ref[...]


def load_matrix(matrix_ref, packed_ref):
    for c in range(WIDTH):
        first = WIDTH - HEIGHT[c]
        matrix_ref[WIDTH * c + first : WIDTH * c + WIDTH, :] = packed_ref[
            START[c] : START[c] + HEIGHT[c], :
        ]


def swap_blocks(pieces, block):
    pieces = list(pieces)
    for bit in (1, 2, 4):
        keep = (block & bit) == 0
        for k in range(T):
            if k & bit == 0:
                first, second = pieces[k], pieces[k | bit]
                pieces[k] = jnp.where(keep, first, pltpu.roll(second, bit * OWN_GENES, 1))
                pieces[k | bit] = jnp.where(
                    keep, pltpu.roll(first, LANES - bit * OWN_GENES, 1), second
                )
    return pieces


def halves(tile, low):
    middle = tile.shape[0] // 2
    top, bottom = tile[:middle], tile[middle:]
    return (
        jnp.where(low, top, pltpu.roll(bottom, HALF, 1)),
        jnp.where(low, pltpu.roll(top, HALF, 1), bottom),
    )


def two_parts(value):
    high = value.astype(BF16)
    return high, (value - high.astype(F32)).astype(BF16)


def matmul_t(left, right):
    return lax.dot_general(left, right, (((1,), (1,)), ((), ())), preferred_element_type=F32)


def kernel(
    counts_hbm, totals_hbm, factors_hbm, loadings_hbm,
    new_factors_ref, new_loadings_ref, deviance_ref,
    counts_v, totals_v, totals_z, factors_v, loadings_v, mirror_v,
    right1, table1, high1, low1, counts_low, sums1, local1_out, local1_in, core_out, core_in,
    packed, matrix, right, column, inverse,
    factor_slots, local2_out, local2_in, table2, high2, low2, sums2, piece_out, piece_in,
    final_out, final_in, final_t,
    input_sem, totals_send, totals_recv, mirror_send, mirror_recv, local1_send, local1_recv, core_send, core_recv,
    factor_send, factor_recv, forward_send, local2_send, local2_recv, piece_send, piece_recv,
    final_send, final_recv,
):
    cell = lax.axis_index("cell")
    gene = lax.axis_index("gene")
    x, z, yh = cell // (Z * YH), (cell // YH) % Z, cell % YH
    yl, core = gene // 2, gene % 2
    t = x * YH + yh
    partner, mirror = yl * 2 + 1 - core, (1 - yl) * 2 + core

    def at(x_, z_, yh_, gene_):
        return {"cell": (x_ * Z + z_) * YH + yh_, "gene": gene_}

    def send(src, dst, send_sem, recv_sem, device):
        return pltpu.make_async_remote_copy(
            src_ref=src, dst_ref=dst, send_sem=send_sem, recv_sem=recv_sem,
            device_id=device, device_id_type=MESH,
        )

    def run(action, first, last):
        def body(k, carry):
            action(k)
            return carry

        lax.fori_loop(first, last, body, 0)

    barrier = pltpu.get_barrier_semaphore()

    def greet(device):
        pl.semaphore_signal(barrier, inc=1, device_id=device, device_id_type=MESH)

    for step in range(1, 4):
        greet(at(x, z, yh, (gene + step) % 4))
    for d in range(1, Z):
        greet(at(x, (z + d) % Z, yh, gene))
    for d in range(1, T):
        greet(at((t + d) % T // YH, z, (t + d) % YH, gene))
    inputs = [
        pltpu.make_async_copy(source, target, input_sem.at[k])
        for k, (source, target) in enumerate(
            [
                (loadings_hbm, loadings_v), (factors_hbm, factors_v),
                (totals_hbm, totals_v), (counts_hbm, counts_v),
            ]
        )
    ]
    for copy in inputs:
        copy.start()
    inputs[0].wait()
    pl.semaphore_wait(barrier, 3 + Z - 1 + T - 1)

    def mirror_copy(k):
        columns = slice(k * CHUNK, (k + 1) * CHUNK)
        return send(
            loadings_v.at[:, columns], mirror_v.at[:, columns],
            mirror_send.at[k], mirror_recv.at[k], at(x, z, yh, mirror),
        )

    def totals_copy(d):
        return send(
            totals_v, totals_z.at[z], totals_send.at[d], totals_recv.at[z],
            at(x, (z + d) % Z, yh, gene),
        )

    def totals_arrived(d):
        slot = totals_z.at[(z + d) % Z]
        return send(
            slot, slot, totals_send.at[d], totals_recv.at[(z + d) % Z],
            at(x, (z + d) % Z, yh, gene),
        )

    chunks = GENES // CHUNK
    for k in range(chunks):
        mirror_copy(k).start()
    for copy in inputs[1:]:
        copy.wait()

    for d in range(1, Z):
        totals_copy(d).start()
    totals_z[z] = totals_v[...]
    lane = lax.broadcasted_iota(jnp.int32, (1, LANES), 1)
    block = lane // OWN_GENES
    low = lane < HALF
    logs = jnp.log(totals_v[...].astype(F32)) - LOG_SCALE

    lanes_yl = pl.ds(pl.multiple_of(yl * LANES, LANES), LANES)
    old_factors = factors_v[:, lanes_yl]
    left1 = left_stack(old_factors, jnp.where(yl == 0, logs[0:1], logs[1:2]))

    def expect(rows, columns, keep):
        write_table(table1, columns, rows)
        stack = right_stack(rows)
        if keep:
            right1[:, columns] = stack
        high1[:, columns], low1[:, columns] = two_parts(jnp.exp(predict(left1, stack)))

    def contract(columns):
        return (
            matmul_t(table1[:, columns], high1[:, columns]),
            matmul_t(table1[TRIANGLE:, columns], low1[:, columns]),
        )

    for k in range(chunks):
        columns = slice(k * CHUNK, (k + 1) * CHUNK)
        expect(loadings_v[:, columns], columns, True)
    main, rest = contract(slice(0, GENES))
    sums1[:TRIANGLE, :] = main[:TRIANGLE]
    sums1[TRIANGLE:, :] = main[TRIANGLE:] + rest

    counts_low[...] = counts_v[...].astype(F32).astype(BF16)
    local1 = matmul_t(table1[TRIANGLE:, :GENES], counts_low[...])
    for pair in range(2):
        packs = halves(local1[:, pair * LANES : (pair + 1) * LANES], low)
        local1_out[2 * pair], local1_out[2 * pair + 1] = packs

    def local1_copy(step):
        target = (gene + step) % 4
        return send(
            local1_out.at[target], local1_in.at[gene],
            local1_send.at[step], local1_recv.at[gene], at(x, z, yh, target),
        )

    def local1_arrived(step):
        source = (gene + step) % 4
        slot = local1_in.at[source]
        return send(
            slot, slot, local1_send.at[step], local1_recv.at[source], at(x, z, yh, source)
        )

    for step in range(1, 4):
        local1_copy(step).start()
    local1_in[gene] = local1_out[gene]

    for part in range(2):
        for k in range(part * chunks // 2, (part + 1) * chunks // 2):
            mirror_copy(k).wait_recv()
            columns = slice(GENES + k * CHUNK, GENES + (k + 1) * CHUNK)
            expect(mirror_v[:, k * CHUNK : (k + 1) * CHUNK], columns, False)
        main, rest = contract(slice(GENES + part * GENES // 2, GENES + (part + 1) * GENES // 2))
        sums1[:TRIANGLE, :] = sums1[:TRIANGLE, :] + main[:TRIANGLE]
        sums1[TRIANGLE:, :] = sums1[TRIANGLE:, :] + main[TRIANGLE:] + rest

    first_pack, second_pack = halves(sums1[...], low)
    core_out[...] = jnp.where(core == 0, second_pack, first_pack)
    core_copy = send(
        core_out, core_in, core_send.at[0], core_recv.at[0], at(x, z, yh, partner)
    )
    core_copy.start()
    own_pack = jnp.where(core == 0, first_pack, second_pack)
    for step in range(1, 4):
        local1_arrived(step).wait_recv()
    counts_pack = local1_in[0] + local1_in[1] + local1_in[2] + local1_in[3]
    old = jnp.where(core == 0, old_factors, pltpu.roll(old_factors, HALF, 1))
    counts_part = jnp.concatenate([counts_pack, pltpu.roll(counts_pack, HALF, 1)], axis=0)
    core_copy.wait_recv()
    total = own_pack + core_in[...]
    middle = ROWS1 // 2
    packed[:middle, :] = total
    packed[middle:ROWS1, :] = pltpu.roll(total, HALF, 1)
    load_matrix(matrix, packed)
    right[...] = counts_part - packed[TRIANGLE:ROWS1, :] - RIDGE * old
    new = old + solve(matrix, right, column, inverse)
    factor_slots[z, gene] = jnp.where(low, new[:16], pltpu.roll(new[16:], HALF, 1))

    own_slot = factor_slots.at[z, gene]
    own_sem = factor_recv.at[z * 4 + gene]

    def near_copy(step):
        return send(
            own_slot, own_slot, factor_send.at[step], own_sem, at(x, z, yh, (gene + step) % 4)
        )

    def far_copy(d, side):
        return send(
            own_slot, own_slot, factor_send.at[4 + 2 * d + side], own_sem,
            at(x, (z + d) % Z, yh, side * 2 + core),
        )

    def slot_arrived(d, source):
        source_z = (z + d) % Z
        slot = factor_slots.at[source_z, source]
        return send(
            slot, slot, factor_send.at[0], factor_recv.at[source_z * 4 + source],
            at(x, z, yh, partner),
        )

    def forward_copy(d, side):
        source_z, source = (z + d) % Z, side * 2 + core
        slot = factor_slots.at[source_z, source]
        return send(
            slot, slot, forward_send.at[2 * d + side], factor_recv.at[source_z * 4 + source],
            at(x, z, yh, partner),
        )

    for step in range(1, 4):
        near_copy(step).start()
    for d in ORDER[1:]:
        for side in range(2):
            far_copy(d, side).start()

    def factors_of(d):
        slot = (z + d) % Z
        tiles = []
        for pair in range(2):
            first, second = factor_slots[slot, 2 * pair], factor_slots[slot, 2 * pair + 1]
            tiles.append(
                jnp.concatenate(
                    [
                        jnp.where(low, first, pltpu.roll(second, HALF, 1)),
                        jnp.where(low, pltpu.roll(first, HALF, 1), second),
                    ],
                    axis=0,
                )
            )
        return jnp.concatenate(tiles, axis=1)

    for step in range(1, 4):
        slot_arrived(0, (gene + step) % 4).wait_recv()
    rows = factors_of(0)
    new_factors_ref[...] = rows
    factors_low = rows.astype(BF16)
    left2 = left_stack(rows, jnp.concatenate([logs[0:1], logs[1:2]], axis=1))
    for k in range(Z):
        columns = slice(k * GENES_Z, (k + 1) * GENES_Z)
        local2_out[k, :WIDTH, :] = jnp.dot(
            factors_low, counts_low[:, columns], preferred_element_type=F32
        )
        counts = counts_v[:, columns].astype(F32)
        linear = predict(left2, right1[:, columns])
        terms = counts * (jnp.log(jnp.maximum(counts, 1.0)) - linear - 1.0)
        local2_out[k, WIDTH:, :] = jnp.sum(terms.reshape(CELLS // 8, 8, LANES), axis=0)

    def local2_copy(d):
        target = (z + d) % Z
        return send(
            local2_out.at[target], local2_in.at[z],
            local2_send.at[d], local2_recv.at[z], at(x, target, yh, gene),
        )

    def local2_arrived(d):
        source = (z + d) % Z
        slot = local2_in.at[source]
        return send(slot, slot, local2_send.at[d], local2_recv.at[source], at(x, source, yh, gene))

    for d in ORDER[1:]:
        local2_copy(d).start()
    local2_in[z] = local2_out[z]

    lanes_z = pl.ds(pl.multiple_of(z * GENES_Z, GENES_Z), GENES_Z)
    right2 = right1[:, lanes_z]
    expected_sum = jnp.zeros((8, LANES), F32)

    def offsets_of(d):
        logs_z = jnp.log(totals_z[(z + d) % Z].astype(F32)) - LOG_SCALE
        return jnp.concatenate([logs_z[0:1], logs_z[1:2]], axis=1)

    for part in range(2):
        for n in range(part * Z // 2, (part + 1) * Z // 2):
            if n > 0:
                for side in range(2):
                    slot_arrived(ORDER[n], side * 2 + core).wait_recv()
                    forward_copy(ORDER[n], side).start()
                for side in range(2):
                    slot_arrived(ORDER[n], side * 2 + 1 - core).wait_recv()
                totals_arrived(ORDER[n]).wait_recv()
            rows = factors_of(ORDER[n])
            columns = slice(n * CELLS, (n + 1) * CELLS)
            write_table(table2, columns, rows)
            expected = jnp.exp(predict(left_stack(rows, offsets_of(ORDER[n])), right2))
            high2[columns, :], low2[columns, :] = two_parts(expected)
            expected_sum = expected_sum + jnp.sum(
                expected.reshape(CELLS // 8, 8, LANES), axis=0
            )
        columns = slice(part * Z // 2 * CELLS, (part + 1) * Z // 2 * CELLS)
        main = jnp.dot(table2[:, columns], high2[columns, :], preferred_element_type=F32)
        rest = jnp.dot(table2[TRIANGLE:, columns], low2[columns, :], preferred_element_type=F32)
        if part == 0:
            sums2[:TRIANGLE, :] = main[:TRIANGLE]
            sums2[TRIANGLE:ROWS1, :] = -main[TRIANGLE:] - rest
        else:
            sums2[:TRIANGLE, :] = sums2[:TRIANGLE, :] + main[:TRIANGLE]
            sums2[TRIANGLE:ROWS1, :] = sums2[TRIANGLE:ROWS1, :] - main[TRIANGLE:] - rest
    run(lambda d: local2_arrived(d).wait_recv(), 1, Z)
    counts_part = local2_in[0]
    for k in range(1, Z):
        counts_part = counts_part + local2_in[k]
    sums2[TRIANGLE:ROWS1, :] = sums2[TRIANGLE:ROWS1, :] + counts_part[:WIDTH]
    sums2[ROWS1 : ROWS1 + 8, :] = counts_part[WIDTH:] + expected_sum
    sums2[ROWS1 + 8 :, :] = jnp.zeros((ROWS2 - ROWS1 - 8, LANES), F32)

    pieces = swap_blocks([sums2[k * PIECE2 : (k + 1) * PIECE2, :] for k in range(T)], block)
    for k in range(T):
        piece_out[k] = pieces[k]

    def piece_copy(d):
        target = (t + d) % T
        return send(
            piece_out.at[target], piece_in.at[t], piece_send.at[d], piece_recv.at[t],
            at(target // YH, z, target % YH, gene),
        )

    def piece_arrived(d):
        source = (t + d) % T
        slot = piece_in.at[source]
        return send(
            slot, slot, piece_send.at[d], piece_recv.at[source],
            at(source // YH, z, source % YH, gene),
        )

    for d in range(1, T):
        piece_copy(d).start()
    piece_in[t] = piece_out[t]
    for d in range(1, T):
        piece_arrived(d).wait_recv()
    total = piece_in[0]
    for k in range(1, T):
        total = total + piece_in[k]
    for k in range(T):
        packed[k * PIECE2 : (k + 1) * PIECE2, :] = (
            total if k == 0 else pltpu.roll(total, LANES - k * OWN_GENES, 1)
        )
    load_matrix(matrix, packed)
    old = loadings_v[:, lanes_z]
    own = old
    for k in range(1, T):
        own = jnp.where(t == k, pltpu.roll(old, LANES - k * OWN_GENES, 1), own)
    right[...] = packed[TRIANGLE:ROWS1, :] - RIDGE * own
    new = own + solve(matrix, right, column, inverse)
    mean = jnp.sum(packed[ROWS1 : ROWS1 + 8, :], axis=0, keepdims=True) * (
        2.0 / (CELLS * CELL_DEVICES)
    )

    message = new[:8]
    for k in range(1, 4):
        message = jnp.where(
            block == k, pltpu.roll(new[8 * k : 8 * k + 8], k * OWN_GENES, 1), message
        )
    row = lax.broadcasted_iota(jnp.int32, (8, LANES), 0)
    shifted = pltpu.roll(pltpu.roll(message, HALF, 1), 4, 0)
    message = jnp.where(low, message, shifted)
    final_out[...] = jnp.where(row < 4, message, jnp.broadcast_to(mean, (8, LANES)))

    used = slice(0, MESSAGE)

    def final_copy(d):
        target = (cell + d) % CELL_DEVICES
        return send(
            final_out.at[used], final_in.at[t, z, used],
            final_send.at[d], final_recv.at[cell], {"cell": target, "gene": gene},
        )

    def final_arrived(d):
        source = (cell + d) % CELL_DEVICES
        source_t = source // (Z * YH) * YH + source % YH
        slot = final_in.at[source_t, (source // YH) % Z, used]
        return send(
            slot, slot, final_send.at[d], final_recv.at[source], {"cell": source, "gene": gene}
        )

    run(lambda d: final_copy(d).start(), 1, CELL_DEVICES)
    final_in[t, z] = final_out[...]
    run(lambda d: final_arrived(d).wait_recv(), 1, CELL_DEVICES)
    row = lax.broadcasted_iota(jnp.int32, (8 * Z, LANES), 0) % 8
    slabs = []
    for k in range(T):
        rows = final_in[k].reshape(8 * Z, LANES)
        turned = pltpu.roll(rows, HALF, 1)
        slabs.append(
            jnp.where(low, jnp.where(row < 4, rows, pltpu.roll(turned, 4, 0)), turned)
        )
    slabs = swap_blocks(slabs, block)
    for j in range(5):
        final_t[j] = slabs[j]
    for k in range(Z):
        eight = slice(8 * k, 8 * k + 8)
        tile = jnp.concatenate([final_t[j, eight, :] for j in range(4)], axis=0)
        new_loadings_ref[:, k * LANES : (k + 1) * LANES] = tile
        deviance_ref[k : k + 1, :] = final_t[4, 8 * k + 4 : 8 * k + 5, :]

    for k in range(chunks):
        mirror_copy(k).wait_send()
    for step in range(1, 4):
        local1_copy(step).wait_send()
        near_copy(step).wait_send()
    core_copy.wait_send()
    for d in range(1, Z):
        for side in range(2):
            far_copy(d, side).wait_send()
            forward_copy(d, side).wait_send()
        local2_copy(d).wait_send()
        totals_copy(d).wait_send()
    for d in range(1, T):
        piece_copy(d).wait_send()
    run(lambda d: final_copy(d).wait_send(), 1, CELL_DEVICES)


def on_device(counts, totals, cell_factors, gene_loadings):
    hbm, vmem = pl.BlockSpec(memory_space=pltpu.HBM), pl.BlockSpec(memory_space=pltpu.VMEM)
    dma = pltpu.SemaphoreType.DMA
    new_factors, new_loadings, deviance = pl.pallas_call(
        kernel,
        out_shape=(
            jax.ShapeDtypeStruct((WIDTH, CELLS), F32),
            jax.ShapeDtypeStruct((WIDTH, GENES), F32),
            jax.ShapeDtypeStruct((Z, LANES), F32),
        ),
        in_specs=[hbm] * 4,
        out_specs=(vmem,) * 3,
        scratch_shapes=[
            pltpu.VMEM((CELLS, GENES), jnp.int32),
            pltpu.VMEM((2, LANES), jnp.int32),
            pltpu.VMEM((Z, 2, LANES), jnp.int32),
            pltpu.VMEM((WIDTH, CELLS), F32),
            pltpu.VMEM((WIDTH, GENES), F32),
            pltpu.VMEM((WIDTH, GENES), F32),
            pltpu.VMEM((6 * WIDTH + 16, GENES), BF16),
            pltpu.VMEM((ROWS1, 2 * GENES), BF16),
            pltpu.VMEM((LANES, 2 * GENES), BF16),
            pltpu.VMEM((LANES, 2 * GENES), BF16),
            pltpu.VMEM((CELLS, GENES), BF16),
            pltpu.VMEM((ROWS1, LANES), F32),
            pltpu.VMEM((4, 16, LANES), F32),
            pltpu.VMEM((4, 16, LANES), F32),
            pltpu.VMEM((ROWS1 // 2, LANES), F32),
            pltpu.VMEM((ROWS1 // 2, LANES), F32),
            pltpu.VMEM((ROWS2, LANES), F32),
            pltpu.VMEM((WIDTH * WIDTH, LANES), F32),
            pltpu.VMEM((WIDTH, LANES), F32),
            pltpu.VMEM((WIDTH, LANES), F32),
            pltpu.VMEM((WIDTH, LANES), F32),
            pltpu.VMEM((Z, 4, 16, LANES), F32),
            pltpu.VMEM((Z, LOCAL, LANES), F32),
            pltpu.VMEM((Z, LOCAL, LANES), F32),
            pltpu.VMEM((ROWS1, Z * CELLS), BF16),
            pltpu.VMEM((Z * CELLS, LANES), BF16),
            pltpu.VMEM((Z * CELLS, LANES), BF16),
            pltpu.VMEM((ROWS2, LANES), F32),
            pltpu.VMEM((T, PIECE2, LANES), F32),
            pltpu.VMEM((T, PIECE2, LANES), F32),
            pltpu.VMEM((8, LANES), F32),
            pltpu.VMEM((T, Z, 8, LANES), F32),
            pltpu.VMEM((5, 8 * Z, LANES), F32),
            dma((4,)), dma((Z,)), dma((Z,)), dma((4,)), dma((4,)), dma((4,)), dma((4,)),
            dma((1,)), dma((1,)), dma((4 + 2 * Z,)), dma((4 * Z,)), dma((2 * Z,)),
            dma((Z,)), dma((Z,)), dma((T,)), dma((T,)),
            dma((CELL_DEVICES,)), dma((CELL_DEVICES,)),
        ],
        compiler_params=pltpu.CompilerParams(
            collective_id=0, has_side_effects=True, vmem_limit_bytes=67043328
        ),
        name="sweep",
    )(counts, totals.reshape(2, LANES), cell_factors.T, gene_loadings.T)
    return new_factors.T, new_loadings.T, deviance.reshape(GENES)


def solution(mesh):
    return jax.shard_map(
        on_device,
        mesh=mesh,
        in_specs=(P("cell", "gene"), P("cell"), P("cell", None), P("gene", None)),
        out_specs=(P("cell", None), P("gene", None), P("gene")),
        check_vma=False,
    )
```

```python
import math

import jax
import jax.numpy as jnp
from jax import lax
from jax.experimental import pallas as pl
from jax.experimental.pallas import tpu as pltpu
from jax.sharding import PartitionSpec as P

F32, BF16 = jnp.float32, jnp.bfloat16
MESH = pl.DeviceIdType.MESH

RIDGE = 1.0
DAMPING = 0.1
LOG_SCALE = math.log(5000.0)

WIDTH = 32
X, Z, YH = 4, 8, 2
CELL_DEVICES = X * Z * YH
T = X * YH
CELLS = 256
GENES = 1024
LANES = 128
GENES_Z = GENES // Z
OWN_GENES = GENES_Z // T
HALF = LANES // 2
CHUNK = 256
ORDER = (0, 1, 7, 2, 6, 3, 5, 4)

HEIGHT = [WIDTH - c // 8 * 8 for c in range(WIDTH)]
START = [sum(HEIGHT[:c]) for c in range(WIDTH)]
TRIANGLE = sum(HEIGHT)
ROWS1 = TRIANGLE + WIDTH
LOCAL = WIDTH + 8
ROWS2 = 704
PIECE2 = ROWS2 // T
MESSAGE = 5


def parts_of(value):
    high = value.astype(BF16).astype(F32)
    rest = value - high
    middle = rest.astype(BF16).astype(F32)
    return high, middle, rest - middle


def left_stack(factors, offset):
    high, middle, low = parts_of(factors)
    row = lax.broadcasted_iota(jnp.int32, (16, factors.shape[1]), 0)
    off_high, off_middle, off_low = parts_of(offset)
    extra = jnp.where(
        row == 0, off_high, jnp.where(row == 1, off_middle, jnp.where(row == 2, off_low, 0.0))
    )
    return jnp.concatenate([high, high, middle, middle, high, low, extra], axis=0).astype(BF16)


def right_stack(loadings):
    high, middle, low = parts_of(loadings)
    extra = jnp.ones((16, loadings.shape[1]), F32)
    return jnp.concatenate([high, middle, high, middle, low, high, extra], axis=0).astype(BF16)


def predict(left, right):
    return lax.dot_general(left, right, (((0,), (0,)), ((), ())), preferred_element_type=F32)


def write_table(table_ref, columns, rows):
    for c in range(0, WIDTH, 2):
        first = c // 8 * 8
        pair = jnp.concatenate(
            [rows[first:] * rows[c : c + 1], rows[first:] * rows[c + 1 : c + 2]], axis=0
        )
        table_ref[START[c] : START[c] + 2 * HEIGHT[c], columns] = pair.astype(BF16)
    table_ref[TRIANGLE : TRIANGLE + WIDTH, columns] = rows.astype(BF16)


def solve(matrix_ref, right_ref, column_ref, inverse_ref):
    for j in range(8, WIDTH):
        for block in range(j // 8):
            matrix_ref[WIDTH * j + 8 * block : WIDTH * j + 8 * block + 8, :] = matrix_ref[
                pl.ds(WIDTH * 8 * block + j, 8, stride=WIDTH), :
            ]
    diagonal = matrix_ref[pl.ds(0, WIDTH, stride=WIDTH + 1), :]
    shift = RIDGE + DAMPING * (jnp.sum(diagonal, axis=0, keepdims=True) / WIDTH)
    matrix_ref[pl.ds(0, WIDTH, stride=WIDTH + 1), :] = diagonal + shift
    row = lax.broadcasted_iota(jnp.int32, (WIDTH, LANES), 0)

    def enter(c, at, slot, first, second):
        column_ref[slot, 0] = first
        pivot = 1.0 / column_ref[slot, 0, pl.ds(at, 1), :]
        inverse_ref[pl.ds(c, 1), :] = pivot
        first_scaled = jnp.where(row == at, 0.0, first * pivot)
        second = second - first_scaled * column_ref[slot, 0, pl.ds(at + 1, 1), :]
        column_ref[slot, 1] = second
        pivot = 1.0 / column_ref[slot, 1, pl.ds(at + 1, 1), :]
        inverse_ref[pl.ds(c + 1, 1), :] = pivot
        return first_scaled, jnp.where(row == at + 1, 0.0, second * pivot)

    scaled = enter(0, 0, 0, matrix_ref[:WIDTH, :], matrix_ref[WIDTH : 2 * WIDTH, :])
    for group in range(WIDTH // 8):

        def step(pair, scaled):
            first, second = scaled
            c, slot = 2 * pair, pair % 2
            after = jnp.minimum(c + 2, WIDTH - 2)

            def reduced(value, j):
                return (
                    value
                    - first * column_ref[slot, 0, pl.ds(j, 1), :]
                    - second * column_ref[slot, 1, pl.ds(j, 1), :]
                )

            start = pl.multiple_of(after * WIDTH, WIDTH)
            scaled_after = enter(
                c + 2, after, 1 - slot,
                reduced(matrix_ref[pl.ds(start, WIDTH), :], after),
                reduced(matrix_ref[pl.ds(start + WIDTH, WIDTH), :], after + 1),
            )
            value = right_ref[...]
            value = value - first * right_ref[pl.ds(c, 1), :]
            right_ref[...] = value
            right_ref[...] = value - second * right_ref[pl.ds(c + 1, 1), :]
            for j in range(8 * group, WIDTH):
                at = slice(WIDTH * j, WIDTH * j + WIDTH)
                matrix_ref[at, :] = reduced(matrix_ref[at, :], j)
            return scaled_after

        scaled = lax.fori_loop(4 * group, 4 * group + 4, step, scaled)
    return right_ref[...] * inverse_ref[:WIDTH, :]


def load_matrix(matrix_ref, packed_ref):
    for c in range(WIDTH):
        first = WIDTH - HEIGHT[c]
        matrix_ref[WIDTH * c + first : WIDTH * c + WIDTH, :] = packed_ref[
            START[c] : START[c] + HEIGHT[c], :
        ]


def swap_blocks(pieces, block):
    pieces = list(pieces)
    for bit in (1, 2, 4):
        keep = (block & bit) == 0
        for k in range(T):
            if k & bit == 0:
                first, second = pieces[k], pieces[k | bit]
                pieces[k] = jnp.where(keep, first, pltpu.roll(second, bit * OWN_GENES, 1))
                pieces[k | bit] = jnp.where(
                    keep, pltpu.roll(first, LANES - bit * OWN_GENES, 1), second
                )
    return pieces


def halves(tile, low):
    middle = tile.shape[0] // 2
    top, bottom = tile[:middle], tile[middle:]
    return (
        jnp.where(low, top, pltpu.roll(bottom, HALF, 1)),
        jnp.where(low, pltpu.roll(top, HALF, 1), bottom),
    )


def two_parts(value):
    high = value.astype(BF16)
    return high, (value - high.astype(F32)).astype(BF16)


def matmul_t(left, right):
    return lax.dot_general(left, right, (((1,), (1,)), ((), ())), preferred_element_type=F32)


def kernel(
    counts_hbm, totals_hbm, factors_hbm, loadings_hbm,
    factors_out_hbm, final_hbm,
    factors_new, counts_v, totals_v, totals_z, factors_v, loadings_v, mirror_v,
    right1, table1, high1, low1, counts_low, sums1, local1_out, local1_in, core_out, core_in,
    packed, matrix, right, column, inverse,
    factor_slots, local2_out, local2_in, local3_out, local3_in, table2, high2, low2, sums2, piece_out, piece_in,
    final_out,
    input_sem, output_sem, totals_send, totals_recv, mirror_send, mirror_recv, local1_send, local1_recv, core_send, core_recv,
    factor_send, factor_recv, forward_send, local2_send, local2_recv, local3_send, local3_recv, piece_send, piece_recv,
    final_send, final_recv,
):
    cell = lax.axis_index("cell")
    gene = lax.axis_index("gene")
    x, z, yh = cell // (Z * YH), (cell // YH) % Z, cell % YH
    yl, core = gene // 2, gene % 2
    t = x * YH + yh
    partner, mirror = yl * 2 + 1 - core, (1 - yl) * 2 + core

    def at(x_, z_, yh_, gene_):
        return {"cell": (x_ * Z + z_) * YH + yh_, "gene": gene_}

    def send(src, dst, send_sem, recv_sem, device):
        return pltpu.make_async_remote_copy(
            src_ref=src, dst_ref=dst, send_sem=send_sem, recv_sem=recv_sem,
            device_id=device, device_id_type=MESH,
        )

    def run(action, first, last):
        def body(k, carry):
            action(k)
            return carry

        lax.fori_loop(first, last, body, 0)

    inputs = [
        pltpu.make_async_copy(source, target, input_sem.at[k])
        for k, (source, target) in enumerate(
            [
                (loadings_hbm, loadings_v), (factors_hbm, factors_v),
                (totals_hbm, totals_v), (counts_hbm, counts_v),
            ]
        )
    ]
    for copy in inputs:
        copy.start()

    barrier = pltpu.get_barrier_semaphore()

    def greet(device):
        pl.semaphore_signal(barrier, inc=1, device_id=device, device_id_type=MESH)

    for step in range(1, 4):
        greet(at(x, z, yh, (gene + step) % 4))
    for d in range(1, Z):
        greet(at(x, (z + d) % Z, yh, gene))
    for d in range(1, T):
        greet(at((t + d) % T // YH, z, (t + d) % YH, gene))
    inputs[0].wait()
    pl.semaphore_wait(barrier, 3 + Z - 1 + T - 1)

    def mirror_copy(k):
        columns = slice(k * CHUNK, (k + 1) * CHUNK)
        return send(
            loadings_v.at[:, columns], mirror_v.at[:, columns],
            mirror_send.at[k], mirror_recv.at[k], at(x, z, yh, mirror),
        )

    def totals_copy(d):
        return send(
            totals_v, totals_z.at[z], totals_send.at[d], totals_recv.at[z],
            at(x, (z + d) % Z, yh, gene),
        )

    def totals_arrived(d):
        slot = totals_z.at[(z + d) % Z]
        return send(
            slot, slot, totals_send.at[d], totals_recv.at[(z + d) % Z],
            at(x, (z + d) % Z, yh, gene),
        )

    chunks = GENES // CHUNK
    for k in range(chunks):
        mirror_copy(k).start()
    for copy in inputs[1:]:
        copy.wait()

    for d in range(1, Z):
        totals_copy(d).start()
    totals_z[z] = totals_v[...]
    lane = lax.broadcasted_iota(jnp.int32, (1, LANES), 1)
    block = lane // OWN_GENES
    low = lane < HALF
    logs = jnp.log(totals_v[...].astype(F32)) - LOG_SCALE

    lanes_yl = pl.ds(pl.multiple_of(yl * LANES, LANES), LANES)
    old_factors = factors_v[:, lanes_yl]
    left1 = left_stack(old_factors, jnp.where(yl == 0, logs[0:1], logs[1:2]))

    def expect(rows, columns, keep):
        write_table(table1, columns, rows)
        stack = right_stack(rows)
        if keep:
            right1[:, columns] = stack
        high1[:, columns], low1[:, columns] = two_parts(jnp.exp(predict(left1, stack)))

    def contract(columns):
        return (
            matmul_t(table1[:, columns], high1[:, columns]),
            matmul_t(table1[TRIANGLE:, columns], low1[:, columns]),
        )

    for k in range(chunks):
        columns = slice(k * CHUNK, (k + 1) * CHUNK)
        expect(loadings_v[:, columns], columns, True)
    main, rest = contract(slice(0, GENES))
    sums1[:TRIANGLE, :] = main[:TRIANGLE]
    sums1[TRIANGLE:, :] = main[TRIANGLE:] + rest

    counts_low[...] = counts_v[...].astype(F32).astype(BF16)
    local1 = matmul_t(table1[TRIANGLE:, :GENES], counts_low[...])
    for pair in range(2):
        packs = halves(local1[:, pair * LANES : (pair + 1) * LANES], low)
        local1_out[2 * pair], local1_out[2 * pair + 1] = packs

    def local1_copy(step):
        target = (gene + step) % 4
        return send(
            local1_out.at[target], local1_in.at[gene],
            local1_send.at[step], local1_recv.at[gene], at(x, z, yh, target),
        )

    def local1_arrived(step):
        source = (gene + step) % 4
        slot = local1_in.at[source]
        return send(
            slot, slot, local1_send.at[step], local1_recv.at[source], at(x, z, yh, source)
        )

    for step in range(1, 4):
        local1_copy(step).start()
    local1_in[gene] = local1_out[gene]

    for part in range(2):
        for k in range(part * chunks // 2, (part + 1) * chunks // 2):
            mirror_copy(k).wait_recv()
            columns = slice(GENES + k * CHUNK, GENES + (k + 1) * CHUNK)
            expect(mirror_v[:, k * CHUNK : (k + 1) * CHUNK], columns, False)
        main, rest = contract(slice(GENES + part * GENES // 2, GENES + (part + 1) * GENES // 2))
        sums1[:TRIANGLE, :] = sums1[:TRIANGLE, :] + main[:TRIANGLE]
        sums1[TRIANGLE:, :] = sums1[TRIANGLE:, :] + main[TRIANGLE:] + rest

    first_pack, second_pack = halves(sums1[...], low)
    core_out[...] = jnp.where(core == 0, second_pack, first_pack)
    core_copy = send(
        core_out, core_in, core_send.at[0], core_recv.at[0], at(x, z, yh, partner)
    )
    core_copy.start()
    own_pack = jnp.where(core == 0, first_pack, second_pack)
    for step in range(1, 4):
        local1_arrived(step).wait_recv()
    counts_pack = local1_in[0] + local1_in[1] + local1_in[2] + local1_in[3]
    old = jnp.where(core == 0, old_factors, pltpu.roll(old_factors, HALF, 1))
    counts_part = jnp.concatenate([counts_pack, pltpu.roll(counts_pack, HALF, 1)], axis=0)
    core_copy.wait_recv()
    total = own_pack + core_in[...]
    middle = ROWS1 // 2
    packed[:middle, :] = total
    packed[middle:ROWS1, :] = pltpu.roll(total, HALF, 1)
    load_matrix(matrix, packed)
    right[...] = counts_part - packed[TRIANGLE:ROWS1, :] - RIDGE * old
    new = old + solve(matrix, right, column, inverse)
    factor_slots[z, gene] = jnp.where(low, new[:16], pltpu.roll(new[16:], HALF, 1))

    own_slot = factor_slots.at[z, gene]
    own_sem = factor_recv.at[z * 4 + gene]

    def near_copy(step):
        return send(
            own_slot, own_slot, factor_send.at[step], own_sem, at(x, z, yh, (gene + step) % 4)
        )

    def far_copy(d, side):
        return send(
            own_slot, own_slot, factor_send.at[4 + 2 * d + side], own_sem,
            at(x, (z + d) % Z, yh, side * 2 + core),
        )

    def slot_arrived(d, source):
        source_z = (z + d) % Z
        slot = factor_slots.at[source_z, source]
        return send(
            slot, slot, factor_send.at[0], factor_recv.at[source_z * 4 + source],
            at(x, z, yh, partner),
        )

    def forward_copy(d, side):
        source_z, source = (z + d) % Z, side * 2 + core
        slot = factor_slots.at[source_z, source]
        return send(
            slot, slot, forward_send.at[2 * d + side], factor_recv.at[source_z * 4 + source],
            at(x, z, yh, partner),
        )

    for step in range(1, 4):
        near_copy(step).start()
    for d in ORDER[1:]:
        for side in range(2):
            far_copy(d, side).start()

    def factors_of(d):
        slot = (z + d) % Z
        tiles = []
        for pair in range(2):
            first, second = factor_slots[slot, 2 * pair], factor_slots[slot, 2 * pair + 1]
            tiles.append(
                jnp.concatenate(
                    [
                        jnp.where(low, first, pltpu.roll(second, HALF, 1)),
                        jnp.where(low, pltpu.roll(first, HALF, 1), second),
                    ],
                    axis=0,
                )
            )
        return jnp.concatenate(tiles, axis=1)

    def forward(first, last):
        for n in range(first, last):
            for side in range(2):
                slot_arrived(ORDER[n], side * 2 + core).wait_recv()
                forward_copy(ORDER[n], side).start()

    for step in range(1, 4):
        slot_arrived(0, (gene + step) % 4).wait_recv()
    forward(1, 3)
    rows = factors_of(0)
    factors_new[...] = rows
    factors_out = pltpu.make_async_copy(factors_new, factors_out_hbm, output_sem.at[0])
    factors_out.start()
    factors_low = rows.astype(BF16)
    left2 = left_stack(rows, jnp.concatenate([logs[0:1], logs[1:2]], axis=1))
    locals2 = []
    for k in range(Z):
        columns = slice(k * GENES_Z, (k + 1) * GENES_Z)
        counts = counts_v[:, columns].astype(F32)
        linear = predict(left2, right1[:, columns])
        terms = counts * (jnp.log(jnp.maximum(counts, 1.0)) - linear - 1.0)
        locals2.append(
            jnp.concatenate(
                [
                    jnp.dot(
                        factors_low, counts_low[:, columns], preferred_element_type=F32
                    ),
                    jnp.sum(terms.reshape(CELLS // 8, 8, LANES), axis=0),
                ],
                axis=0,
            )
        )
    locals2 = swap_blocks(locals2, block)
    for k in range(T):
        local2_out[k] = locals2[k]

    def local2_copy(d):
        target = (t + d) % T
        return send(
            local2_out.at[target], local2_in.at[t], local2_send.at[d], local2_recv.at[t],
            at(target // YH, z, target % YH, gene),
        )

    def local2_arrived(d):
        source = (t + d) % T
        slot = local2_in.at[source]
        return send(
            slot, slot, local2_send.at[d], local2_recv.at[source],
            at(source // YH, z, source % YH, gene),
        )

    def local3_copy(d):
        target = (z + d) % Z
        return send(
            local3_out.at[target], local3_in.at[z], local3_send.at[d], local3_recv.at[z],
            at(x, target, yh, gene),
        )

    def local3_arrived(d):
        source = (z + d) % Z
        slot = local3_in.at[source]
        return send(slot, slot, local3_send.at[d], local3_recv.at[source], at(x, source, yh, gene))

    for d in range(1, T):
        local2_copy(d).start()
    local2_in[t] = local2_out[t]

    right2 = right1[:, pl.ds(pl.multiple_of(z * GENES_Z, GENES_Z), GENES_Z)]

    def offsets_of(d):
        logs_z = jnp.log(totals_z[(z + d) % Z].astype(F32)) - LOG_SCALE
        return jnp.concatenate([logs_z[0:1], logs_z[1:2]], axis=1)

    def expect2(first, last):
        for n in range(max(first, 1), last):
            for side in range(2):
                slot_arrived(ORDER[n], side * 2 + 1 - core).wait_recv()
            totals_arrived(ORDER[n]).wait_recv()
        rows = jnp.concatenate([factors_of(ORDER[n]) for n in range(first, last)], axis=1)
        offsets = jnp.concatenate([offsets_of(ORDER[n]) for n in range(first, last)], axis=1)
        columns = slice(first * CELLS, last * CELLS)
        write_table(table2, columns, rows)
        expected = jnp.exp(predict(left_stack(rows, offsets), right2))
        high2[columns, :], low2[columns, :] = two_parts(expected)
        return jnp.sum(expected.reshape((last - first) * CELLS // 8, 8, LANES), axis=0)

    def contract2(first, last):
        columns = slice(first * CELLS, last * CELLS)
        main = jnp.dot(table2[:, columns], high2[columns, :], preferred_element_type=F32)
        rest = jnp.dot(table2[TRIANGLE:, columns], low2[columns, :], preferred_element_type=F32)
        if first == 0:
            sums2[:TRIANGLE, :] = main[:TRIANGLE]
            sums2[TRIANGLE:ROWS1, :] = main[TRIANGLE:] + rest
        else:
            sums2[:TRIANGLE, :] = sums2[:TRIANGLE, :] + main[:TRIANGLE]
            sums2[TRIANGLE:ROWS1, :] = sums2[TRIANGLE:ROWS1, :] + main[TRIANGLE:] + rest

    expected_sum = expect2(0, 1)
    forward(3, 5)
    expected_sum = expected_sum + expect2(1, 3)
    forward(5, 7)
    expected_sum = expected_sum + expect2(3, 5)
    forward(7, 8)
    contract2(0, 5)
    expected_sum = expected_sum + expect2(5, 7)
    expected_sum = expected_sum + expect2(7, 8)
    contract2(5, 8)
    sums2[ROWS1 : ROWS1 + 8, :] = expected_sum
    sums2[ROWS1 + 8 :, :] = jnp.zeros((ROWS2 - ROWS1 - 8, LANES), F32)

    pieces = swap_blocks([sums2[k * PIECE2 : (k + 1) * PIECE2, :] for k in range(T)], block)
    for k in range(T):
        piece_out[k] = pieces[k]

    def piece_copy(d):
        target = (t + d) % T
        return send(
            piece_out.at[target], piece_in.at[t], piece_send.at[d], piece_recv.at[t],
            at(target // YH, z, target % YH, gene),
        )

    def piece_arrived(d):
        source = (t + d) % T
        slot = piece_in.at[source]
        return send(
            slot, slot, piece_send.at[d], piece_recv.at[source],
            at(source // YH, z, source % YH, gene),
        )

    for d in range(1, T):
        piece_copy(d).start()
    piece_in[t] = piece_out[t]
    for d in range(1, T):
        local2_arrived(d).wait_recv()
    counts_sum = local2_in[0]
    for k in range(1, T):
        counts_sum = counts_sum + local2_in[k]
    zero = jnp.zeros((8, LANES), F32)
    pieces = [counts_sum[8 * k : 8 * k + 8] for k in range(LOCAL // 8)]
    pieces = swap_blocks(pieces + [zero] * (Z - LOCAL // 8), block)
    for k in range(Z):
        local3_out[k] = pieces[k]
    for d in range(1, Z):
        local3_copy(d).start()
    local3_in[z] = local3_out[z]
    for d in ORDER[1:]:
        local3_arrived(d).wait_recv()
    counts_sum = local3_in[0]
    for k in range(1, Z):
        counts_sum = counts_sum + local3_in[k]
    counts_sum = [counts_sum] + [
        pltpu.roll(counts_sum, LANES - k * OWN_GENES, 1) for k in range(1, LOCAL // 8)
    ]
    for d in range(1, T):
        piece_arrived(d).wait_recv()
    total = piece_in[0]
    for k in range(1, T):
        total = total + piece_in[k]
    for k in range(T):
        packed[k * PIECE2 : (k + 1) * PIECE2, :] = (
            total if k == 0 else pltpu.roll(total, LANES - k * OWN_GENES, 1)
        )
    load_matrix(matrix, packed)
    old = loadings_v[:, pl.ds(pl.multiple_of(z * GENES_Z, GENES_Z), GENES_Z)]
    own = old
    for k in range(1, T):
        own = jnp.where(t == k, pltpu.roll(old, LANES - k * OWN_GENES, 1), own)
    right[...] = jnp.concatenate(counts_sum[:4], axis=0) - packed[TRIANGLE:ROWS1, :] - RIDGE * own
    new = own + solve(matrix, right, column, inverse)
    mean = jnp.sum(packed[ROWS1 : ROWS1 + 8, :] + counts_sum[4], axis=0, keepdims=True) * (
        2.0 / (CELLS * CELL_DEVICES)
    )

    message = new[:8]
    for k in range(1, 4):
        message = jnp.where(
            block == k, pltpu.roll(new[8 * k : 8 * k + 8], k * OWN_GENES, 1), message
        )
    row = lax.broadcasted_iota(jnp.int32, (8, LANES), 0)
    shifted = pltpu.roll(pltpu.roll(message, HALF, 1), 4, 0)
    message = jnp.where(low, message, shifted)
    final_out[...] = jnp.where(row < 4, message, jnp.broadcast_to(mean, (8, LANES)))

    used = slice(0, MESSAGE)

    places = [(dx, dz, dy) for dx in range(X) for dz in range(Z) for dy in range(YH)]
    places.sort(key=lambda p: -(min(p[0], X - p[0]) + min(p[1], Z - p[1]) + 2 * p[2]))
    places = places[:-1]
    xs = [(x + d) % X for d in range(X)]
    zs = [(z + d) % Z for d in range(Z)]
    ys = [(yh + d) % YH for d in range(YH)]

    def cell_of(place):
        return (xs[place[0]] * Z + zs[place[1]]) * YH + ys[place[2]]

    def final_copy(k):
        return send(
            final_out.at[used], final_hbm.at[t, z, used], final_send.at[k], final_recv.at[cell],
            {"cell": cell_of(places[k]), "gene": gene},
        )

    def final_arrived(k):
        dx, dz, dy = places[k]
        slot = final_hbm.at[xs[dx] * YH + ys[dy], zs[dz], used]
        source = cell_of(places[k])
        return send(
            slot, slot, final_send.at[k], final_recv.at[source], {"cell": source, "gene": gene}
        )

    for k in range(len(places)):
        final_copy(k).start()
    own_final = pltpu.make_async_copy(
        final_out.at[used], final_hbm.at[t, z, used], output_sem.at[1]
    )
    own_final.start()

    for k in range(chunks):
        mirror_copy(k).wait_send()
    for step in range(1, 4):
        local1_copy(step).wait_send()
        near_copy(step).wait_send()
    core_copy.wait_send()
    for d in range(1, Z):
        for side in range(2):
            far_copy(d, side).wait_send()
            forward_copy(d, side).wait_send()
        local3_copy(d).wait_send()
        totals_copy(d).wait_send()
    for d in range(1, T):
        local2_copy(d).wait_send()
        piece_copy(d).wait_send()
    factors_out.wait()
    own_final.wait()
    for k in range(len(places)):
        final_copy(k).wait_send()
    for k in reversed(range(len(places))):
        final_arrived(k).wait_recv()


def unpack(final_ref, factors_ref, new_factors_ref, new_loadings_ref, deviance_ref):
    new_factors_ref[...] = factors_ref[...]
    lane = lax.broadcasted_iota(jnp.int32, (1, LANES), 1)
    row = lax.broadcasted_iota(jnp.int32, (8 * Z, LANES), 0) % 8
    low = lane < HALF
    slabs = []
    for k in range(T):
        rows = final_ref[k].reshape(8 * Z, LANES)
        turned = pltpu.roll(rows, HALF, 1)
        slabs.append(
            jnp.where(low, jnp.where(row < 4, rows, pltpu.roll(turned, 4, 0)), turned)
        )
    slabs = swap_blocks(slabs, lane // OWN_GENES)
    for k in range(Z):
        eight = slice(8 * k, 8 * k + 8)
        tile = jnp.concatenate([slabs[j][eight] for j in range(4)], axis=0)
        new_loadings_ref[:, k * LANES : (k + 1) * LANES] = tile
        deviance_ref[k : k + 1, :] = slabs[4][8 * k + 4 : 8 * k + 5]


def on_device(counts, totals, cell_factors, gene_loadings):
    hbm, vmem = pl.BlockSpec(memory_space=pltpu.HBM), pl.BlockSpec(memory_space=pltpu.VMEM)
    dma = pltpu.SemaphoreType.DMA
    factors_new, final = pl.pallas_call(
        kernel,
        out_shape=(
            jax.ShapeDtypeStruct((WIDTH, CELLS), F32),
            jax.ShapeDtypeStruct((T, Z, 8, LANES), F32),
        ),
        in_specs=[hbm] * 4,
        out_specs=(hbm,) * 2,
        scratch_shapes=[
            pltpu.VMEM((WIDTH, CELLS), F32),
            pltpu.VMEM((CELLS, GENES), jnp.int32),
            pltpu.VMEM((2, LANES), jnp.int32),
            pltpu.VMEM((Z, 2, LANES), jnp.int32),
            pltpu.VMEM((WIDTH, CELLS), F32),
            pltpu.VMEM((WIDTH, GENES), F32),
            pltpu.VMEM((WIDTH, GENES), F32),
            pltpu.VMEM((6 * WIDTH + 16, GENES), BF16),
            pltpu.VMEM((ROWS1, 2 * GENES), BF16),
            pltpu.VMEM((LANES, 2 * GENES), BF16),
            pltpu.VMEM((LANES, 2 * GENES), BF16),
            pltpu.VMEM((CELLS, GENES), BF16),
            pltpu.VMEM((ROWS1, LANES), F32),
            pltpu.VMEM((4, 16, LANES), F32),
            pltpu.VMEM((4, 16, LANES), F32),
            pltpu.VMEM((ROWS1 // 2, LANES), F32),
            pltpu.VMEM((ROWS1 // 2, LANES), F32),
            pltpu.VMEM((ROWS2, LANES), F32),
            pltpu.VMEM((WIDTH * WIDTH, LANES), F32),
            pltpu.VMEM((WIDTH, LANES), F32),
            pltpu.VMEM((2, 2, WIDTH, LANES), F32),
            pltpu.VMEM((WIDTH + 8, LANES), F32),
            pltpu.VMEM((Z, 4, 16, LANES), F32),
            pltpu.VMEM((T, LOCAL, LANES), F32),
            pltpu.VMEM((T, LOCAL, LANES), F32),
            pltpu.VMEM((Z, 8, LANES), F32),
            pltpu.VMEM((Z, 8, LANES), F32),
            pltpu.VMEM((ROWS1, Z * CELLS), BF16),
            pltpu.VMEM((Z * CELLS, LANES), BF16),
            pltpu.VMEM((Z * CELLS, LANES), BF16),
            pltpu.VMEM((ROWS2, LANES), F32),
            pltpu.VMEM((T, PIECE2, LANES), F32),
            pltpu.VMEM((T, PIECE2, LANES), F32),
            pltpu.VMEM((8, LANES), F32),
            dma((4,)), dma((2,)), dma((Z,)), dma((Z,)), dma((4,)), dma((4,)), dma((4,)), dma((4,)),
            dma((1,)), dma((1,)), dma((4 + 2 * Z,)), dma((4 * Z,)), dma((2 * Z,)),
            dma((T,)), dma((T,)), dma((Z,)), dma((Z,)), dma((T,)), dma((T,)),
            dma((CELL_DEVICES,)), dma((CELL_DEVICES,)),
        ],
        compiler_params=pltpu.CompilerParams(
            collective_id=0, has_side_effects=True, vmem_limit_bytes=67043328
        ),
        name="sweep",
    )(counts, totals.reshape(2, LANES), cell_factors.T, gene_loadings.T)
    new_factors, new_loadings, deviance = pl.pallas_call(
        unpack,
        out_shape=(
            jax.ShapeDtypeStruct((WIDTH, CELLS), F32),
            jax.ShapeDtypeStruct((WIDTH, GENES), F32),
            jax.ShapeDtypeStruct((Z, LANES), F32),
        ),
        in_specs=[vmem] * 2,
        out_specs=(vmem,) * 3,
        name="unpack",
    )(final, factors_new)
    return new_factors.T, new_loadings.T, deviance.reshape(GENES)


def solution(mesh):
    return jax.shard_map(
        on_device,
        mesh=mesh,
        in_specs=(P("cell", "gene"), P("cell"), P("cell", None), P("gene", None)),
        out_specs=(P("cell", None), P("gene", None), P("gene")),
        check_vma=False,
    )
```

```python
import math

import jax
import jax.numpy as jnp
from jax import lax
from jax.experimental import pallas as pl
from jax.experimental.pallas import tpu as pltpu
from jax.sharding import PartitionSpec as P

F32, BF16 = jnp.float32, jnp.bfloat16
MESH = pl.DeviceIdType.MESH

RIDGE = 1.0
DAMPING = 0.1
LOG_SCALE = math.log(5000.0)

WIDTH = 32
X, Z, YH = 4, 8, 2
CELL_DEVICES = X * Z * YH
T = X * YH
CELLS = 256
GENES = 1024
LANES = 128
GENES_Z = GENES // Z
OWN_GENES = GENES_Z // T
HALF = LANES // 2
CHUNK = 128
ORDER = (0, 1, 7, 2, 6, 3, 5, 4)
FAR_FIRST = ORDER[:0:-1]
PLANE = ((0, 0), (2, 1), (1, 1), (3, 1), (2, 0), (0, 1), (1, 0), (3, 0))

HEIGHT = [WIDTH - c // 8 * 8 for c in range(WIDTH)]
START = [sum(HEIGHT[:c]) for c in range(WIDTH)]
TRIANGLE = sum(HEIGHT)
ROWS1 = TRIANGLE + WIDTH
LOCAL = WIDTH + 8
ROWS2 = 704
MESSAGE = 5


def parts_of(value):
    high = value.astype(BF16).astype(F32)
    rest = value - high
    middle = rest.astype(BF16).astype(F32)
    return high, middle, rest - middle


def left_stack(factors, offset):
    high, middle, low = parts_of(factors)
    row = lax.broadcasted_iota(jnp.int32, (16, factors.shape[1]), 0)
    off_high, off_middle, off_low = parts_of(offset)
    extra = jnp.where(
        row == 0, off_high, jnp.where(row == 1, off_middle, jnp.where(row == 2, off_low, 0.0))
    )
    return jnp.concatenate([high, high, middle, middle, high, low, extra], axis=0).astype(BF16)


def right_stack(loadings):
    high, middle, low = parts_of(loadings)
    extra = jnp.ones((16, loadings.shape[1]), F32)
    return jnp.concatenate([high, middle, high, middle, low, high, extra], axis=0).astype(BF16)


def predict(left, right):
    return lax.dot_general(left, right, (((0,), (0,)), ((), ())), preferred_element_type=F32)


def write_table(table_ref, columns, rows):
    for c in range(0, WIDTH, 2):
        first = c // 8 * 8
        pair = jnp.concatenate(
            [rows[first:] * rows[c : c + 1], rows[first:] * rows[c + 1 : c + 2]], axis=0
        )
        table_ref[START[c] : START[c] + 2 * HEIGHT[c], columns] = pair.astype(BF16)
    table_ref[TRIANGLE : TRIANGLE + WIDTH, columns] = rows.astype(BF16)


def solve(matrix_ref, right_ref, first_ref, second_ref, inverse_ref):
    for j in range(8, WIDTH):
        for block in range(j // 8):
            matrix_ref[WIDTH * j + 8 * block : WIDTH * j + 8 * block + 8, :] = matrix_ref[
                pl.ds(WIDTH * 8 * block + j, 8, stride=WIDTH), :
            ]
    diagonal = matrix_ref[pl.ds(0, WIDTH, stride=WIDTH + 1), :]
    shift = RIDGE + DAMPING * (jnp.sum(diagonal, axis=0, keepdims=True) / WIDTH)
    matrix_ref[pl.ds(0, WIDTH, stride=WIDTH + 1), :] = diagonal + shift
    row = lax.broadcasted_iota(jnp.int32, (WIDTH, LANES), 0)

    def enter(c, at, column_ref, first, second):
        column_ref[0] = first
        pivot = 1.0 / column_ref[0, pl.ds(at, 1), :]
        inverse_ref[pl.ds(c, 1), :] = pivot
        first_scaled = jnp.where(row == at, 0.0, first * pivot)
        second = second - first_scaled * column_ref[0, pl.ds(at + 1, 1), :]
        column_ref[1] = second
        pivot = 1.0 / column_ref[1, pl.ds(at + 1, 1), :]
        inverse_ref[pl.ds(c + 1, 1), :] = pivot
        return first_scaled, jnp.where(row == at + 1, 0.0, second * pivot)

    def advance(c, scaled, column_ref, column_next_ref, group):
        first, second = scaled
        after = jnp.minimum(c + 2, WIDTH - 2)

        def reduced(value, j):
            return (
                value
                - first * column_ref[0, pl.ds(j, 1), :]
                - second * column_ref[1, pl.ds(j, 1), :]
            )

        start = pl.multiple_of(after * WIDTH, WIDTH)
        scaled_after = enter(
            c + 2, after, column_next_ref,
            reduced(matrix_ref[pl.ds(start, WIDTH), :], after),
            reduced(matrix_ref[pl.ds(start + WIDTH, WIDTH), :], after + 1),
        )
        value = right_ref[...]
        value = value - first * right_ref[pl.ds(c, 1), :]
        right_ref[...] = value
        right_ref[...] = value - second * right_ref[pl.ds(c + 1, 1), :]
        for j in range(8 * group, WIDTH):
            at = slice(WIDTH * j, WIDTH * j + WIDTH)
            matrix_ref[at, :] = reduced(matrix_ref[at, :], j)
        return scaled_after

    scaled = enter(0, 0, first_ref, matrix_ref[:WIDTH, :], matrix_ref[WIDTH : 2 * WIDTH, :])
    for group in range(WIDTH // 8):

        def step(quad, scaled):
            scaled = advance(4 * quad, scaled, first_ref, second_ref, group)
            return advance(4 * quad + 2, scaled, second_ref, first_ref, group)

        scaled = lax.fori_loop(2 * group, 2 * group + 2, step, scaled)
    return right_ref[...] * inverse_ref[:WIDTH, :]


def load_matrix(matrix_ref, packed_ref):
    for c in range(WIDTH):
        first = WIDTH - HEIGHT[c]
        matrix_ref[WIDTH * c + first : WIDTH * c + WIDTH, :] = packed_ref[
            START[c] : START[c] + HEIGHT[c], :
        ]


def swap_blocks(pieces, block):
    pieces = list(pieces)
    for bit in (1, 2, 4):
        keep = (block & bit) == 0
        for k in range(T):
            if k & bit == 0:
                first, second = pieces[k], pieces[k | bit]
                pieces[k] = jnp.where(keep, first, pltpu.roll(second, bit * OWN_GENES, 1))
                pieces[k | bit] = jnp.where(
                    keep, pltpu.roll(first, LANES - bit * OWN_GENES, 1), second
                )
    return pieces


def halves(tile, low):
    middle = tile.shape[0] // 2
    top, bottom = tile[:middle], tile[middle:]
    return (
        jnp.where(low, top, pltpu.roll(bottom, HALF, 1)),
        jnp.where(low, pltpu.roll(top, HALF, 1), bottom),
    )


def two_parts(value):
    high = value.astype(BF16)
    return high, (value - high.astype(F32)).astype(BF16)


def matmul_t(left, right):
    return lax.dot_general(left, right, (((1,), (1,)), ((), ())), preferred_element_type=F32)


def kernel(
    counts_hbm, totals_hbm, factors_hbm, loadings_hbm,
    factors_out_hbm, final_hbm,
    factors_new, counts_v, totals_v, totals_z, factors_v, loadings_v, mirror_v,
    right1, table1, high1, low1, counts_low, sums1, local1_out, local1_in, core_out, core_in,
    packed, matrix, right, column_a, column_b, inverse,
    factor_slots, local2_out, local2_in, local3_out, local3_in, table2, high2, low2, sums2, bases,
    piece_out_a, piece_in_a, piece_out_b, piece_in_b,
    final_out,
    rounds, input_sem, output_sem, totals_send, totals_recv, mirror_send, mirror_recv, local1_send, local1_recv, core_send, core_recv,
    factor_send, factor_recv, forward_send, local2_send, local2_recv, local3_send, local3_recv, piece_send, piece_recv,
    final_send, final_recv,
):
    cell = lax.axis_index("cell")
    gene = lax.axis_index("gene")
    x, z, yh = cell // (Z * YH), (cell // YH) % Z, cell % YH
    yl, core = gene // 2, gene % 2
    t = x * YH + yh
    partner, mirror = yl * 2 + 1 - core, (1 - yl) * 2 + core

    def at(x_, z_, yh_, gene_):
        return {"cell": (x_ * Z + z_) * YH + yh_, "gene": gene_}

    def plane(k):
        return (x + PLANE[k][0]) % X * YH + (yh + PLANE[k][1]) % YH

    def send(src, dst, send_sem, recv_sem, device):
        return pltpu.make_async_remote_copy(
            src_ref=src, dst_ref=dst, send_sem=send_sem, recv_sem=recv_sem,
            device_id=device, device_id_type=MESH,
        )

    def run(action, first, last):
        def body(k, carry):
            action(k)
            return carry

        lax.fori_loop(first, last, body, 0)

    inputs = [
        pltpu.make_async_copy(source, target, input_sem.at[k])
        for k, (source, target) in enumerate(
            [
                (loadings_hbm, loadings_v), (factors_hbm, factors_v),
                (totals_hbm, totals_v), (counts_hbm, counts_v),
            ]
        )
    ]
    for copy in inputs:
        copy.start()

    barrier = pltpu.get_barrier_semaphore()

    def greet(device):
        pl.semaphore_signal(barrier, inc=1, device_id=device, device_id_type=MESH)

    for step in range(1, 4):
        greet(at(x, z, yh, (gene + step) % 4))
    greet(at(x, z, 1 - yh, mirror))
    greet(at(x, z, 1 - yh, gene))
    steps_z, steps_x = (1, Z - 1, 2, Z - 2), (1, X - 1, 2)
    for d in steps_z:
        greet(at(x, (z + d) % Z, yh, gene))
    for d in steps_x:
        greet(at((x + d) % X, z, yh, gene))

    def tell(first, devices):
        for k, device in enumerate(devices):
            pl.semaphore_signal(
                rounds.at[first + k], inc=1, device_id=device, device_id_type=MESH
            )

    def told(first, last):
        for k in range(first, last):
            pl.semaphore_wait(rounds.at[k], 1)

    inputs[0].wait()
    pl.semaphore_wait(barrier, 12)
    tell(0, [at(x, (z + d) % Z, yh, gene) for d in steps_z])
    tell(6, [at((x + d) % X, z, yh, gene) for d in steps_x])

    chunks = GENES // CHUNK

    def mirror_copy(k):
        columns = slice(k * CHUNK, (k + 1) * CHUNK)
        return send(
            loadings_v.at[:, columns], mirror_v.at[:, columns],
            mirror_send.at[k], mirror_recv.at[k],
            at(x, z, yh if k < chunks // 2 else 1 - yh, mirror),
        )

    def totals_copy(d):
        return send(
            totals_v, totals_z.at[z], totals_send.at[d], totals_recv.at[z],
            at(x, (z + d) % Z, yh, gene),
        )

    def totals_arrived(d):
        slot = totals_z.at[(z + d) % Z]
        return send(
            slot, slot, totals_send.at[d], totals_recv.at[(z + d) % Z],
            at(x, (z + d) % Z, yh, gene),
        )

    arrival = [k // 2 + k % 2 * (chunks // 2) for k in range(chunks)]
    for k in arrival:
        mirror_copy(k).start()
    for copy in inputs[1:]:
        copy.wait()

    totals_z[z] = totals_v[...]
    lane = lax.broadcasted_iota(jnp.int32, (1, LANES), 1)
    block = lane // OWN_GENES
    low = lane < HALF
    logs = jnp.log(totals_v[...].astype(F32)) - LOG_SCALE

    lanes_yl = pl.ds(pl.multiple_of(yl * LANES, LANES), LANES)
    old_factors = factors_v[:, lanes_yl]
    left1 = left_stack(old_factors, jnp.where(yl == 0, logs[0:1], logs[1:2]))

    def expect(rows, columns, keep):
        write_table(table1, columns, rows)
        stack = right_stack(rows)
        if keep:
            right1[:, columns] = stack
        high1[:, columns], low1[:, columns] = two_parts(jnp.exp(predict(left1, stack)))

    def contract(columns):
        return (
            matmul_t(table1[:, columns], high1[:, columns]),
            matmul_t(table1[TRIANGLE:, columns], low1[:, columns]),
        )

    for k in range(0, chunks, 2):
        columns = slice(k * CHUNK, (k + 2) * CHUNK)
        expect(loadings_v[:, columns], columns, True)
    main, rest = contract(slice(0, GENES))
    sums1[:TRIANGLE, :] = main[:TRIANGLE]
    sums1[TRIANGLE:, :] = main[TRIANGLE:] + rest

    counts_low[...] = counts_v[...].astype(F32).astype(BF16)
    local1 = matmul_t(table1[TRIANGLE:, :GENES], counts_low[...])
    for pair in range(2):
        packs = halves(local1[:, pair * LANES : (pair + 1) * LANES], low)
        local1_out[2 * pair], local1_out[2 * pair + 1] = packs

    def local1_copy(step):
        target = (gene + step) % 4
        return send(
            local1_out.at[target], local1_in.at[gene],
            local1_send.at[step], local1_recv.at[gene], at(x, z, yh, target),
        )

    def local1_arrived(step):
        source = (gene + step) % 4
        slot = local1_in.at[source]
        return send(
            slot, slot, local1_send.at[step], local1_recv.at[source], at(x, z, yh, source)
        )

    for step in range(1, 4):
        local1_copy(step).start()
    local1_in[gene] = local1_out[gene]

    for k in range(0, chunks, 2):
        for n in range(k, k + 2):
            mirror_copy(arrival[n]).wait_recv()
        rows = jnp.concatenate(
            [mirror_v[:, n * CHUNK : (n + 1) * CHUNK] for n in arrival[k : k + 2]], axis=1
        )
        columns = slice(GENES + k * CHUNK, GENES + (k + 2) * CHUNK)
        expect(rows, columns, False)
        main, rest = contract(columns)
        sums1[:TRIANGLE, :] = sums1[:TRIANGLE, :] + main[:TRIANGLE]
        sums1[TRIANGLE:, :] = sums1[TRIANGLE:, :] + main[TRIANGLE:] + rest

    first_pack, second_pack = halves(sums1[...], low)
    core_out[...] = jnp.where(core == 0, second_pack, first_pack)
    core_copy = send(
        core_out, core_in, core_send.at[0], core_recv.at[0], at(x, z, yh, partner)
    )
    core_copy.start()
    told(0, 4)
    tell(4, [at(x, (z + d) % Z, yh, gene) for d in steps_z[2:]])
    own_pack = jnp.where(core == 0, first_pack, second_pack)
    for step in range(1, 4):
        local1_arrived(step).wait_recv()
    counts_pack = local1_in[0] + local1_in[1] + local1_in[2] + local1_in[3]
    old = jnp.where(core == 0, old_factors, pltpu.roll(old_factors, HALF, 1))
    counts_part = jnp.concatenate([counts_pack, pltpu.roll(counts_pack, HALF, 1)], axis=0)
    core_copy.wait_recv()
    total = own_pack + core_in[...]
    middle = ROWS1 // 2
    packed[:middle, :] = total
    packed[middle:ROWS1, :] = pltpu.roll(total, HALF, 1)
    load_matrix(matrix, packed)
    right[...] = counts_part - packed[TRIANGLE:ROWS1, :] - RIDGE * old
    new = old + solve(matrix, right, column_a, column_b, inverse)
    factor_slots[z, gene] = jnp.where(low, new[:16], pltpu.roll(new[16:], HALF, 1))

    own_slot = factor_slots.at[z, gene]
    own_sem = factor_recv.at[z * 4 + gene]

    def near_copy(step):
        return send(
            own_slot, own_slot, factor_send.at[step], own_sem, at(x, z, yh, (gene + step) % 4)
        )

    def far_copy(d, side):
        return send(
            own_slot, own_slot, factor_send.at[4 + 2 * d + side], own_sem,
            at(x, (z + d) % Z, yh, side * 2 + core),
        )

    def slot_arrived(d, source):
        source_z = (z + d) % Z
        slot = factor_slots.at[source_z, source]
        return send(
            slot, slot, factor_send.at[0], factor_recv.at[source_z * 4 + source],
            at(x, z, yh, partner),
        )

    def forward_copy(d, side):
        source_z, source = (z + d) % Z, side * 2 + core
        slot = factor_slots.at[source_z, source]
        return send(
            slot, slot, forward_send.at[2 * d + side], factor_recv.at[source_z * 4 + source],
            at(x, z, yh, partner),
        )

    for step in range(1, 4):
        near_copy(step).start()
    told(4, 6)
    for d in FAR_FIRST:
        for side in range(2):
            far_copy(d, side).start()
    for d in FAR_FIRST:
        totals_copy(d).start()

    def factors_of(d):
        slot = (z + d) % Z
        tiles = []
        for pair in range(2):
            first, second = factor_slots[slot, 2 * pair], factor_slots[slot, 2 * pair + 1]
            tiles.append(
                jnp.concatenate(
                    [
                        jnp.where(low, first, pltpu.roll(second, HALF, 1)),
                        jnp.where(low, pltpu.roll(first, HALF, 1), second),
                    ],
                    axis=0,
                )
            )
        return jnp.concatenate(tiles, axis=1)

    def forward(first, last):
        for n in range(first, last):
            for side in range(2):
                slot_arrived(ORDER[n], side * 2 + core).wait_recv()
                forward_copy(ORDER[n], side).start()

    for k in range(Z):
        counts = counts_v[:, k * GENES_Z : (k + 1) * GENES_Z].astype(F32)
        terms = counts * (jnp.log(jnp.maximum(counts, 1.0)) - 1.0)
        bases[k] = jnp.sum(terms.reshape(CELLS // 8, 8, LANES), axis=0)
    for step in range(1, 4):
        slot_arrived(0, (gene + step) % 4).wait_recv()
    rows = factors_of(0)
    factors_new[...] = rows
    factors_out = pltpu.make_async_copy(factors_new, factors_out_hbm, output_sem.at[0])
    factors_out.start()
    factor_parts = parts_of(rows)
    offset_parts = parts_of(jnp.concatenate([logs[0:1], logs[1:2]], axis=1))
    row = lax.broadcasted_iota(jnp.int32, (16, CELLS), 0)
    extra = jnp.zeros((16, CELLS), F32)
    for k in range(3):
        extra = jnp.where(row == k, offset_parts[k], extra)
    left2 = jnp.concatenate([*factor_parts, extra], axis=0).astype(BF16)
    row = lax.broadcasted_iota(jnp.int32, (8, LANES), 0)
    locals2 = []
    for k in range(Z):
        columns = slice(k * GENES_Z, (k + 1) * GENES_Z)
        product = jnp.dot(left2, counts_low[:, columns], preferred_element_type=F32)
        gradient = product[:WIDTH]
        weighted = loadings_v[:, columns] * (
            gradient + product[WIDTH : 2 * WIDTH] + product[2 * WIDTH : 3 * WIDTH]
        )
        linear = jnp.where(row < 3, product[3 * WIDTH : 3 * WIDTH + 8], 0.0)
        for n in range(WIDTH // 8):
            linear = linear + weighted[8 * n : 8 * n + 8]
        locals2.append(jnp.concatenate([gradient, bases[k] - linear], axis=0))
    locals2 = swap_blocks(locals2, block)
    for k in range(T):
        local2_out[k] = locals2[k]

    def local2_copy(d):
        target = plane(d)
        return send(
            local2_out.at[target], local2_in.at[t], local2_send.at[d], local2_recv.at[t],
            at(target // YH, z, target % YH, gene),
        )

    def local2_arrived(d):
        source = plane(d)
        slot = local2_in.at[source]
        return send(
            slot, slot, local2_send.at[d], local2_recv.at[source],
            at(source // YH, z, source % YH, gene),
        )

    def local3_copy(d):
        target = (z + d) % Z
        return send(
            local3_out.at[target], local3_in.at[z], local3_send.at[d], local3_recv.at[z],
            at(x, target, yh, gene),
        )

    def local3_arrived(d):
        source = (z + d) % Z
        slot = local3_in.at[source]
        return send(slot, slot, local3_send.at[d], local3_recv.at[source], at(x, source, yh, gene))

    told(6, 9)
    for d in range(1, T):
        local2_copy(d).start()
    local2_in[t] = local2_out[t]

    right2 = right1[:, pl.ds(pl.multiple_of(z * GENES_Z, GENES_Z), GENES_Z)]

    def offsets_of(d):
        logs_z = jnp.log(totals_z[(z + d) % Z].astype(F32)) - LOG_SCALE
        return jnp.concatenate([logs_z[0:1], logs_z[1:2]], axis=1)

    def wait2(first, last):
        for n in range(first, last):
            for side in range(2):
                slot_arrived(ORDER[n], side * 2 + 1 - core).wait_recv()
            totals_arrived(ORDER[n]).wait_recv()

    def expect2(first, last):
        rows = jnp.concatenate([factors_of(ORDER[n]) for n in range(first, last)], axis=1)
        offsets = jnp.concatenate([offsets_of(ORDER[n]) for n in range(first, last)], axis=1)
        columns = slice(first * CELLS, last * CELLS)
        write_table(table2, columns, rows)
        expected = jnp.exp(predict(left_stack(rows, offsets), right2))
        high2[columns, :], low2[columns, :] = two_parts(expected)
        return jnp.sum(expected.reshape((last - first) * CELLS // 8, 8, LANES), axis=0)

    def contract2(first, last, top, bottom):
        columns = slice(first * CELLS, last * CELLS)
        rows = slice(top, bottom)
        main = jnp.dot(table2[rows, columns], high2[columns, :], preferred_element_type=F32)
        sums2[rows, :] = main if first == 0 else sums2[rows, :] + main
        if bottom == ROWS1:
            sums2[TRIANGLE:ROWS1, :] = sums2[TRIANGLE:ROWS1, :] + jnp.dot(
                table2[TRIANGLE:, columns], low2[columns, :], preferred_element_type=F32
            )

    forward(1, 3)
    expected_sum = expect2(0, 1)
    forward(3, 5)
    wait2(1, 3)
    expected_sum = expected_sum + expect2(1, 3)
    forward(5, 7)
    contract2(0, 3, 0, ROWS1)
    forward(7, 8)
    wait2(3, 5)
    expected_sum = expected_sum + expect2(3, 5)
    wait2(5, 7)
    contract2(3, 5, 0, ROWS1)
    expected_sum = expected_sum + expect2(5, 7)
    wait2(7, 8)
    contract2(5, 7, 0, ROWS1)
    expected_sum = expected_sum + expect2(7, 8)
    sums2[ROWS1 : ROWS1 + 8, :] = expected_sum
    sums2[ROWS1 + 8 :, :] = jnp.zeros((ROWS2 - ROWS1 - 8, LANES), F32)

    parts = ((0, 48, piece_out_a, piece_in_a), (T * 48, 40, piece_out_b, piece_in_b))

    def piece_copy(part, d):
        target = plane(d)
        return send(
            parts[part][2].at[target], parts[part][3].at[t],
            piece_send.at[part * T + d], piece_recv.at[part * T + t],
            at(target // YH, z, target % YH, gene),
        )

    def piece_arrived(part, d):
        source = plane(d)
        slot = parts[part][3].at[source]
        return send(
            slot, slot, piece_send.at[part * T + d], piece_recv.at[part * T + source],
            at(source // YH, z, source % YH, gene),
        )

    for part, (top, height, out_ref, in_ref) in enumerate(parts):
        contract2(7, 8, top, min(top + T * height, ROWS1))
        rows = [sums2[top + k * height : top + (k + 1) * height, :] for k in range(T)]
        rows = swap_blocks(rows, block)
        for k in range(T):
            out_ref[k] = rows[k]
        for d in range(1, T):
            piece_copy(part, d).start()
        in_ref[t] = out_ref[t]
    for d in range(1, T):
        local2_arrived(d).wait_recv()
    counts_sum = local2_in[0]
    for k in range(1, T):
        counts_sum = counts_sum + local2_in[k]
    zero = jnp.zeros((8, LANES), F32)
    pieces = [counts_sum[8 * k : 8 * k + 8] for k in range(LOCAL // 8)]
    pieces = swap_blocks(pieces + [zero] * (Z - LOCAL // 8), block)
    for k in range(Z):
        local3_out[k] = pieces[k]
    for d in FAR_FIRST:
        local3_copy(d).start()
    local3_in[z] = local3_out[z]
    for d in ORDER[1:]:
        local3_arrived(d).wait_recv()
    counts_sum = local3_in[0]
    for k in range(1, Z):
        counts_sum = counts_sum + local3_in[k]
    counts_sum = [counts_sum] + [
        pltpu.roll(counts_sum, LANES - k * OWN_GENES, 1) for k in range(1, LOCAL // 8)
    ]
    for part, (top, height, out_ref, in_ref) in enumerate(parts):
        for d in range(1, T):
            piece_arrived(part, d).wait_recv()
        total = in_ref[0]
        for k in range(1, T):
            total = total + in_ref[k]
        for k in range(T):
            packed[top + k * height : top + (k + 1) * height, :] = (
                total if k == 0 else pltpu.roll(total, LANES - k * OWN_GENES, 1)
            )
    load_matrix(matrix, packed)
    old = loadings_v[:, pl.ds(pl.multiple_of(z * GENES_Z, GENES_Z), GENES_Z)]
    own = old
    for k in range(1, T):
        own = jnp.where(t == k, pltpu.roll(old, LANES - k * OWN_GENES, 1), own)
    right[...] = jnp.concatenate(counts_sum[:4], axis=0) - packed[TRIANGLE:ROWS1, :] - RIDGE * own
    new = own + solve(matrix, right, column_a, column_b, inverse)
    mean = jnp.sum(packed[ROWS1 : ROWS1 + 8, :] + counts_sum[4], axis=0, keepdims=True) * (
        2.0 / (CELLS * CELL_DEVICES)
    )

    message = new[:8]
    for k in range(1, 4):
        message = jnp.where(
            block == k, pltpu.roll(new[8 * k : 8 * k + 8], k * OWN_GENES, 1), message
        )
    row = lax.broadcasted_iota(jnp.int32, (8, LANES), 0)
    shifted = pltpu.roll(pltpu.roll(message, HALF, 1), 4, 0)
    message = jnp.where(low, message, shifted)
    final_out[...] = jnp.where(row < 4, message, jnp.broadcast_to(mean, (8, LANES)))

    used = slice(0, MESSAGE)

    places = [(dx, dz, dy) for dx in range(X) for dz in range(Z) for dy in range(YH)]
    places.sort(key=lambda p: -(min(p[0], X - p[0]) + min(p[1], Z - p[1]) + 2 * p[2]))
    places = places[:-1]
    xs = [(x + d) % X for d in range(X)]
    zs = [(z + d) % Z for d in range(Z)]
    ys = [(yh + d) % YH for d in range(YH)]

    def cell_of(place):
        return (xs[place[0]] * Z + zs[place[1]]) * YH + ys[place[2]]

    def final_copy(k):
        return send(
            final_out.at[used], final_hbm.at[t, z, used], final_send.at[k], final_recv.at[cell],
            {"cell": cell_of(places[k]), "gene": gene},
        )

    def final_arrived(k):
        dx, dz, dy = places[k]
        slot = final_hbm.at[xs[dx] * YH + ys[dy], zs[dz], used]
        source = cell_of(places[k])
        return send(
            slot, slot, final_send.at[k], final_recv.at[source], {"cell": source, "gene": gene}
        )

    for k in range(len(places)):
        final_copy(k).start()
    own_final = pltpu.make_async_copy(
        final_out.at[used], final_hbm.at[t, z, used], output_sem.at[1]
    )
    own_final.start()

    for k in range(chunks):
        mirror_copy(k).wait_send()
    for step in range(1, 4):
        local1_copy(step).wait_send()
        near_copy(step).wait_send()
    core_copy.wait_send()
    for d in range(1, Z):
        for side in range(2):
            far_copy(d, side).wait_send()
            forward_copy(d, side).wait_send()
        local3_copy(d).wait_send()
        totals_copy(d).wait_send()
    for d in range(1, T):
        local2_copy(d).wait_send()
        piece_copy(0, d).wait_send()
        piece_copy(1, d).wait_send()
    factors_out.wait()
    own_final.wait()
    for k in range(len(places)):
        final_copy(k).wait_send()
    for k in reversed(range(len(places))):
        final_arrived(k).wait_recv()


def unpack(final_ref, factors_ref, new_factors_ref, new_loadings_ref, deviance_ref):
    new_factors_ref[...] = factors_ref[...]
    lane = lax.broadcasted_iota(jnp.int32, (1, LANES), 1)
    row = lax.broadcasted_iota(jnp.int32, (8 * Z, LANES), 0) % 8
    low = lane < HALF
    slabs = []
    for k in range(T):
        rows = final_ref[k].reshape(8 * Z, LANES)
        turned = pltpu.roll(rows, HALF, 1)
        slabs.append(
            jnp.where(low, jnp.where(row < 4, rows, pltpu.roll(turned, 4, 0)), turned)
        )
    slabs = swap_blocks(slabs, lane // OWN_GENES)
    for k in range(Z):
        eight = slice(8 * k, 8 * k + 8)
        tile = jnp.concatenate([slabs[j][eight] for j in range(4)], axis=0)
        new_loadings_ref[:, k * LANES : (k + 1) * LANES] = tile
        deviance_ref[k : k + 1, :] = slabs[4][8 * k + 4 : 8 * k + 5]


def on_device(counts, totals, cell_factors, gene_loadings):
    hbm, vmem = pl.BlockSpec(memory_space=pltpu.HBM), pl.BlockSpec(memory_space=pltpu.VMEM)
    dma = pltpu.SemaphoreType.DMA
    factors_new, final = pl.pallas_call(
        kernel,
        out_shape=(
            jax.ShapeDtypeStruct((WIDTH, CELLS), F32),
            jax.ShapeDtypeStruct((T, Z, 8, LANES), F32),
        ),
        in_specs=[hbm] * 4,
        out_specs=(hbm,) * 2,
        scratch_shapes=[
            pltpu.VMEM((WIDTH, CELLS), F32),
            pltpu.VMEM((CELLS, GENES), jnp.int32),
            pltpu.VMEM((2, LANES), jnp.int32),
            pltpu.VMEM((Z, 2, LANES), jnp.int32),
            pltpu.VMEM((WIDTH, CELLS), F32),
            pltpu.VMEM((WIDTH, GENES), F32),
            pltpu.VMEM((WIDTH, GENES), F32),
            pltpu.VMEM((6 * WIDTH + 16, GENES), BF16),
            pltpu.VMEM((ROWS1, 2 * GENES), BF16),
            pltpu.VMEM((LANES, 2 * GENES), BF16),
            pltpu.VMEM((LANES, 2 * GENES), BF16),
            pltpu.VMEM((CELLS, GENES), BF16),
            pltpu.VMEM((ROWS1, LANES), F32),
            pltpu.VMEM((4, 16, LANES), F32),
            pltpu.VMEM((4, 16, LANES), F32),
            pltpu.VMEM((ROWS1 // 2, LANES), F32),
            pltpu.VMEM((ROWS1 // 2, LANES), F32),
            pltpu.VMEM((ROWS2, LANES), F32),
            pltpu.VMEM((WIDTH * WIDTH, LANES), F32),
            pltpu.VMEM((WIDTH, LANES), F32),
            pltpu.VMEM((2, WIDTH, LANES), F32),
            pltpu.VMEM((2, WIDTH, LANES), F32),
            pltpu.VMEM((WIDTH + 8, LANES), F32),
            pltpu.VMEM((Z, 4, 16, LANES), F32),
            pltpu.VMEM((T, LOCAL, LANES), F32),
            pltpu.VMEM((T, LOCAL, LANES), F32),
            pltpu.VMEM((Z, 8, LANES), F32),
            pltpu.VMEM((Z, 8, LANES), F32),
            pltpu.VMEM((ROWS1, Z * CELLS), BF16),
            pltpu.VMEM((Z * CELLS, LANES), BF16),
            pltpu.VMEM((Z * CELLS, LANES), BF16),
            pltpu.VMEM((ROWS2, LANES), F32),
            pltpu.VMEM((Z, 8, LANES), F32),
            pltpu.VMEM((T, 48, LANES), F32),
            pltpu.VMEM((T, 48, LANES), F32),
            pltpu.VMEM((T, 40, LANES), F32),
            pltpu.VMEM((T, 40, LANES), F32),
            pltpu.VMEM((8, LANES), F32),
            pltpu.SemaphoreType.REGULAR((9,)),
            dma((4,)), dma((2,)), dma((Z,)), dma((Z,)), dma((8,)), dma((8,)), dma((4,)), dma((4,)),
            dma((1,)), dma((1,)), dma((4 + 2 * Z,)), dma((4 * Z,)), dma((2 * Z,)),
            dma((T,)), dma((T,)), dma((Z,)), dma((Z,)), dma((2 * T,)), dma((2 * T,)),
            dma((CELL_DEVICES,)), dma((CELL_DEVICES,)),
        ],
        compiler_params=pltpu.CompilerParams(
            collective_id=0, has_side_effects=True, vmem_limit_bytes=67043328
        ),
        name="sweep",
    )(counts, totals.reshape(2, LANES), cell_factors.T, gene_loadings.T)
    new_factors, new_loadings, deviance = pl.pallas_call(
        unpack,
        out_shape=(
            jax.ShapeDtypeStruct((WIDTH, CELLS), F32),
            jax.ShapeDtypeStruct((WIDTH, GENES), F32),
            jax.ShapeDtypeStruct((Z, LANES), F32),
        ),
        in_specs=[vmem] * 2,
        out_specs=(vmem,) * 3,
        name="unpack",
    )(final, factors_new)
    return new_factors.T, new_loadings.T, deviance.reshape(GENES)


def solution(mesh):
    return jax.shard_map(
        on_device,
        mesh=mesh,
        in_specs=(P("cell", "gene"), P("cell"), P("cell", None), P("gene", None)),
        out_specs=(P("cell", None), P("gene", None), P("gene")),
        check_vma=False,
    )
```

```python
import math

import jax
import jax.numpy as jnp
from jax import lax
from jax.experimental import pallas as pl
from jax.experimental.pallas import tpu as pltpu
from jax.sharding import PartitionSpec as P

F32, BF16 = jnp.float32, jnp.bfloat16
MESH = pl.DeviceIdType.MESH

RIDGE = 1.0
DAMPING = 0.1
LOG_SCALE = math.log(5000.0)

WIDTH = 32
X, Z, YH = 4, 8, 2
CELL_DEVICES = X * Z * YH
T = X * YH
CELLS = 256
GENES = 1024
LANES = 128
GENES_Z = GENES // Z
OWN_GENES = GENES_Z // T
HALF = LANES // 2
CHUNK = 128
ORDER = (0, 1, 7, 3, 5, 4, 2, 6)
FAR_FIRST = (4, 3, 5, 2, 6, 1, 7)
SENT = (1, 7, 4, 3, 5, 2, 6)
PLANE = ((0, 0), (2, 1), (1, 1), (3, 1), (2, 0), (0, 1), (1, 0), (3, 0))

HEIGHT = [WIDTH - c // 8 * 8 for c in range(WIDTH)]
START = [sum(HEIGHT[:c]) for c in range(WIDTH)]
TRIANGLE = sum(HEIGHT)
ROWS1 = TRIANGLE + WIDTH
LOCAL = WIDTH + 8
ROWS2 = 704
MESSAGE = 5


def parts_of(value):
    high = value.astype(BF16).astype(F32)
    rest = value - high
    middle = rest.astype(BF16).astype(F32)
    return high, middle, rest - middle


def left_stack(factors, offset):
    high, middle, low = parts_of(factors)
    row = lax.broadcasted_iota(jnp.int32, (16, factors.shape[1]), 0)
    off_high, off_middle, off_low = parts_of(offset)
    extra = jnp.where(
        row == 0, off_high, jnp.where(row == 1, off_middle, jnp.where(row == 2, off_low, 0.0))
    )
    return jnp.concatenate([high, high, middle, middle, high, low, extra], axis=0).astype(BF16)


def right_stack(loadings):
    high, middle, low = parts_of(loadings)
    extra = jnp.ones((16, loadings.shape[1]), F32)
    return jnp.concatenate([high, middle, high, middle, low, high, extra], axis=0).astype(BF16)


def predict(left, right):
    return lax.dot_general(left, right, (((0,), (0,)), ((), ())), preferred_element_type=F32)


def write_table(table_ref, columns, rows):
    for c in range(0, WIDTH, 2):
        first = c // 8 * 8
        pair = jnp.concatenate(
            [rows[first:] * rows[c : c + 1], rows[first:] * rows[c + 1 : c + 2]], axis=0
        )
        table_ref[START[c] : START[c] + 2 * HEIGHT[c], columns] = pair.astype(BF16)
    table_ref[TRIANGLE : TRIANGLE + WIDTH, columns] = rows.astype(BF16)


def solve(matrix_ref, right_ref, first_ref, second_ref, inverse_ref):
    for j in range(8, WIDTH):
        for block in range(j // 8):
            matrix_ref[WIDTH * j + 8 * block : WIDTH * j + 8 * block + 8, :] = matrix_ref[
                pl.ds(WIDTH * 8 * block + j, 8, stride=WIDTH), :
            ]
    diagonal = matrix_ref[pl.ds(0, WIDTH, stride=WIDTH + 1), :]
    shift = RIDGE + DAMPING * (jnp.sum(diagonal, axis=0, keepdims=True) / WIDTH)
    matrix_ref[pl.ds(0, WIDTH, stride=WIDTH + 1), :] = diagonal + shift
    row = lax.broadcasted_iota(jnp.int32, (WIDTH, LANES), 0)

    def enter(c, column_ref, first, second):
        column_ref[0] = first
        pivot = 1.0 / column_ref[0, c : c + 1, :]
        inverse_ref[c : c + 1, :] = pivot
        first_scaled = jnp.where(row == c, 0.0, first * pivot)
        second = second - first_scaled * column_ref[0, c + 1 : c + 2, :]
        column_ref[1] = second
        pivot = 1.0 / column_ref[1, c + 1 : c + 2, :]
        inverse_ref[c + 1 : c + 2, :] = pivot
        return first_scaled, jnp.where(row == c + 1, 0.0, second * pivot)

    first, second = enter(0, first_ref, matrix_ref[:WIDTH, :], matrix_ref[WIDTH : 2 * WIDTH, :])
    for c in range(0, WIDTH, 2):
        column_ref, other_ref = (first_ref, second_ref) if c % 4 == 0 else (second_ref, first_ref)

        def reduced(j):
            return (
                matrix_ref[WIDTH * j : WIDTH * j + WIDTH, :]
                - first * column_ref[0, j : j + 1, :]
                - second * column_ref[1, j : j + 1, :]
            )

        if c + 2 < WIDTH:
            after = enter(c + 2, other_ref, reduced(c + 2), reduced(c + 3))
        value = right_ref[...]
        value = value - first * right_ref[c : c + 1, :]
        right_ref[...] = value
        right_ref[...] = value - second * right_ref[c + 1 : c + 2, :]
        for j in range(c + 4, WIDTH):
            matrix_ref[WIDTH * j : WIDTH * j + WIDTH, :] = reduced(j)
        if c + 2 < WIDTH:
            first, second = after
    return right_ref[...] * inverse_ref[:WIDTH, :]


def load_matrix(matrix_ref, packed_ref):
    for c in range(WIDTH):
        first = WIDTH - HEIGHT[c]
        matrix_ref[WIDTH * c + first : WIDTH * c + WIDTH, :] = packed_ref[
            START[c] : START[c] + HEIGHT[c], :
        ]


def swap_blocks(pieces, block):
    pieces = list(pieces)
    for bit in (1, 2, 4):
        keep = (block & bit) == 0
        for k in range(T):
            if k & bit == 0:
                first, second = pieces[k], pieces[k | bit]
                pieces[k] = jnp.where(keep, first, pltpu.roll(second, bit * OWN_GENES, 1))
                pieces[k | bit] = jnp.where(
                    keep, pltpu.roll(first, LANES - bit * OWN_GENES, 1), second
                )
    return pieces


def halves(tile, low):
    middle = tile.shape[0] // 2
    top, bottom = tile[:middle], tile[middle:]
    return (
        jnp.where(low, top, pltpu.roll(bottom, HALF, 1)),
        jnp.where(low, pltpu.roll(top, HALF, 1), bottom),
    )


def two_parts(value):
    high = value.astype(BF16)
    return high, (value - high.astype(F32)).astype(BF16)


def matmul_t(left, right):
    return lax.dot_general(left, right, (((1,), (1,)), ((), ())), preferred_element_type=F32)


def kernel(
    counts_hbm, totals_hbm, factors_hbm, loadings_hbm,
    factors_out_hbm, final_hbm,
    factors_new, counts_v, totals_v, totals_z, factors_v, loadings_v, mirror_v,
    right1, table1, high1, low1, counts_low, sums1, local1_out, local1_in, core_out, core_in,
    packed, matrix, right, column_a, column_b, inverse,
    factor_slots, local2_out, local2_in, local3_out, local3_in, table2, high2, low2, sums2, bases,
    piece_out_a, piece_in_a, piece_out_b, piece_in_b,
    final_out,
    rounds, input_sem, output_sem, totals_send, totals_recv, mirror_send, mirror_recv, local1_send, local1_recv, core_send, core_recv,
    factor_send, factor_recv, forward_send, local2_send, local2_recv, local3_send, local3_recv, piece_send, piece_recv,
    final_send, final_recv,
):
    cell = lax.axis_index("cell")
    gene = lax.axis_index("gene")
    x, z, yh = cell // (Z * YH), (cell // YH) % Z, cell % YH
    yl, core = gene // 2, gene % 2
    t = x * YH + yh
    partner, mirror = yl * 2 + 1 - core, (1 - yl) * 2 + core

    def at(x_, z_, yh_, gene_):
        return {"cell": (x_ * Z + z_) * YH + yh_, "gene": gene_}

    def plane(k):
        return (x + PLANE[k][0]) % X * YH + (yh + PLANE[k][1]) % YH

    def send(src, dst, send_sem, recv_sem, device):
        return pltpu.make_async_remote_copy(
            src_ref=src, dst_ref=dst, send_sem=send_sem, recv_sem=recv_sem,
            device_id=device, device_id_type=MESH,
        )

    def run(action, first, last):
        def body(k, carry):
            action(k)
            return carry

        lax.fori_loop(first, last, body, 0)

    inputs = [
        pltpu.make_async_copy(source, target, input_sem.at[k])
        for k, (source, target) in enumerate(
            [
                (loadings_hbm, loadings_v), (factors_hbm, factors_v),
                (totals_hbm, totals_v), (counts_hbm, counts_v),
            ]
        )
    ]
    for copy in inputs:
        copy.start()

    barrier = pltpu.get_barrier_semaphore()

    def greet(device):
        pl.semaphore_signal(barrier, inc=1, device_id=device, device_id_type=MESH)

    for step in range(1, 4):
        greet(at(x, z, yh, (gene + step) % 4))
    greet(at(x, z, 1 - yh, mirror))
    greet(at(x, z, 1 - yh, gene))
    steps_z, steps_x = (1, Z - 1, 2, Z - 2), (1, X - 1, 2)
    for d in steps_z:
        greet(at(x, (z + d) % Z, yh, gene))
    for d in steps_x:
        greet(at((x + d) % X, z, yh, gene))

    def tell(first, devices):
        for k, device in enumerate(devices):
            pl.semaphore_signal(
                rounds.at[first + k], inc=1, device_id=device, device_id_type=MESH
            )

    def told(first, last):
        for k in range(first, last):
            pl.semaphore_wait(rounds.at[k], 1)

    inputs[0].wait()
    pl.semaphore_wait(barrier, 12)
    tell(0, [at(x, (z + d) % Z, yh, gene) for d in steps_z])
    tell(6, [at((x + d) % X, z, yh, gene) for d in steps_x])

    chunks = GENES // CHUNK

    def mirror_copy(k):
        columns = slice(k * CHUNK, (k + 1) * CHUNK)
        return send(
            loadings_v.at[:, columns], mirror_v.at[:, columns],
            mirror_send.at[k], mirror_recv.at[k],
            at(x, z, yh if k < chunks // 2 else 1 - yh, mirror),
        )

    def totals_copy(d):
        return send(
            totals_v, totals_z.at[z], totals_send.at[d], totals_recv.at[z],
            at(x, (z + d) % Z, yh, gene),
        )

    def totals_arrived(d):
        slot = totals_z.at[(z + d) % Z]
        return send(
            slot, slot, totals_send.at[d], totals_recv.at[(z + d) % Z],
            at(x, (z + d) % Z, yh, gene),
        )

    arrival = [k // 2 + k % 2 * (chunks // 2) for k in range(chunks)]
    for k in arrival:
        mirror_copy(k).start()
    for copy in inputs[1:]:
        copy.wait()

    totals_z[z] = totals_v[...]
    lane = lax.broadcasted_iota(jnp.int32, (1, LANES), 1)
    block = lane // OWN_GENES
    low = lane < HALF
    logs = jnp.log(totals_v[...].astype(F32)) - LOG_SCALE

    lanes_yl = pl.ds(pl.multiple_of(yl * LANES, LANES), LANES)
    old_factors = factors_v[:, lanes_yl]
    left1 = left_stack(old_factors, jnp.where(yl == 0, logs[0:1], logs[1:2]))

    def expect(rows, columns, keep):
        write_table(table1, columns, rows)
        stack = right_stack(rows)
        if keep:
            right1[:, columns] = stack
        high1[:, columns], low1[:, columns] = two_parts(jnp.exp(predict(left1, stack)))

    def contract(columns):
        return (
            matmul_t(table1[:, columns], high1[:, columns]),
            matmul_t(table1[TRIANGLE:, columns], low1[:, columns]),
        )

    for k in range(0, chunks, 2):
        columns = slice(k * CHUNK, (k + 2) * CHUNK)
        expect(loadings_v[:, columns], columns, True)
    main, rest = contract(slice(0, GENES))
    sums1[:TRIANGLE, :] = main[:TRIANGLE]
    sums1[TRIANGLE:, :] = main[TRIANGLE:] + rest

    counts_low[...] = counts_v[...].astype(F32).astype(BF16)
    local1 = matmul_t(table1[TRIANGLE:, :GENES], counts_low[...])
    for pair in range(2):
        packs = halves(local1[:, pair * LANES : (pair + 1) * LANES], low)
        local1_out[2 * pair], local1_out[2 * pair + 1] = packs

    def local1_copy(step):
        target = (gene + step) % 4
        return send(
            local1_out.at[target], local1_in.at[gene],
            local1_send.at[step], local1_recv.at[gene], at(x, z, yh, target),
        )

    def local1_arrived(step):
        source = (gene + step) % 4
        slot = local1_in.at[source]
        return send(
            slot, slot, local1_send.at[step], local1_recv.at[source], at(x, z, yh, source)
        )

    for step in range(1, 4):
        local1_copy(step).start()
    local1_in[gene] = local1_out[gene]

    for k in range(0, chunks, 2):
        for n in range(k, k + 2):
            mirror_copy(arrival[n]).wait_recv()
        rows = jnp.concatenate(
            [mirror_v[:, n * CHUNK : (n + 1) * CHUNK] for n in arrival[k : k + 2]], axis=1
        )
        columns = slice(GENES + k * CHUNK, GENES + (k + 2) * CHUNK)
        expect(rows, columns, False)
        main, rest = contract(columns)
        sums1[:TRIANGLE, :] = sums1[:TRIANGLE, :] + main[:TRIANGLE]
        sums1[TRIANGLE:, :] = sums1[TRIANGLE:, :] + main[TRIANGLE:] + rest

    first_pack, second_pack = halves(sums1[...], low)
    core_out[...] = jnp.where(core == 0, second_pack, first_pack)
    core_copy = send(
        core_out, core_in, core_send.at[0], core_recv.at[0], at(x, z, yh, partner)
    )
    core_copy.start()
    told(0, 4)
    tell(4, [at(x, (z + d) % Z, yh, gene) for d in steps_z[2:]])
    own_pack = jnp.where(core == 0, first_pack, second_pack)
    for step in range(1, 4):
        local1_arrived(step).wait_recv()
    counts_pack = local1_in[0] + local1_in[1] + local1_in[2] + local1_in[3]
    old = jnp.where(core == 0, old_factors, pltpu.roll(old_factors, HALF, 1))
    counts_part = jnp.concatenate([counts_pack, pltpu.roll(counts_pack, HALF, 1)], axis=0)
    core_copy.wait_recv()
    total = own_pack + core_in[...]
    middle = ROWS1 // 2
    packed[:middle, :] = total
    packed[middle:ROWS1, :] = pltpu.roll(total, HALF, 1)
    load_matrix(matrix, packed)
    right[...] = counts_part - packed[TRIANGLE:ROWS1, :] - RIDGE * old
    new = old + solve(matrix, right, column_a, column_b, inverse)
    factor_slots[z, gene] = jnp.where(low, new[:16], pltpu.roll(new[16:], HALF, 1))

    own_slot = factor_slots.at[z, gene]
    own_sem = factor_recv.at[z * 4 + gene]

    def near_copy(step):
        return send(
            own_slot, own_slot, factor_send.at[step], own_sem, at(x, z, yh, (gene + step) % 4)
        )

    def far_copy(d, side):
        return send(
            own_slot, own_slot, factor_send.at[4 + 2 * d + side], own_sem,
            at(x, (z + d) % Z, yh, side * 2 + core),
        )

    def slot_arrived(d, source):
        source_z = (z + d) % Z
        slot = factor_slots.at[source_z, source]
        return send(
            slot, slot, factor_send.at[0], factor_recv.at[source_z * 4 + source],
            at(x, z, yh, partner),
        )

    def forward_copy(d, side):
        source_z, source = (z + d) % Z, side * 2 + core
        slot = factor_slots.at[source_z, source]
        return send(
            slot, slot, forward_send.at[2 * d + side], factor_recv.at[source_z * 4 + source],
            at(x, z, yh, partner),
        )

    for step in range(1, 4):
        near_copy(step).start()
    told(4, 6)
    for d in SENT:
        for side in range(2):
            far_copy(d, side).start()
    for d in SENT:
        totals_copy(d).start()

    def factors_of(d):
        slot = (z + d) % Z
        tiles = []
        for pair in range(2):
            first, second = factor_slots[slot, 2 * pair], factor_slots[slot, 2 * pair + 1]
            tiles.append(
                jnp.concatenate(
                    [
                        jnp.where(low, first, pltpu.roll(second, HALF, 1)),
                        jnp.where(low, pltpu.roll(first, HALF, 1), second),
                    ],
                    axis=0,
                )
            )
        return jnp.concatenate(tiles, axis=1)

    def forward(first, last):
        for n in range(first, last):
            for side in range(2):
                slot_arrived(ORDER[n], side * 2 + core).wait_recv()
                forward_copy(ORDER[n], side).start()

    for k in range(Z):
        counts = counts_v[:, k * GENES_Z : (k + 1) * GENES_Z].astype(F32)
        terms = counts * (jnp.log(jnp.maximum(counts, 1.0)) - 1.0)
        bases[k] = jnp.sum(terms.reshape(CELLS // 8, 8, LANES), axis=0)
    for step in range(1, 4):
        slot_arrived(0, (gene + step) % 4).wait_recv()
    rows = factors_of(0)
    factors_new[...] = rows
    factors_out = pltpu.make_async_copy(factors_new, factors_out_hbm, output_sem.at[0])
    factors_out.start()
    factor_parts = parts_of(rows)
    offset_parts = parts_of(jnp.concatenate([logs[0:1], logs[1:2]], axis=1))
    row = lax.broadcasted_iota(jnp.int32, (16, CELLS), 0)
    extra = jnp.zeros((16, CELLS), F32)
    for k in range(3):
        extra = jnp.where(row == k, offset_parts[k], extra)
    left2 = jnp.concatenate([*factor_parts, extra], axis=0).astype(BF16)
    row = lax.broadcasted_iota(jnp.int32, (8, LANES), 0)
    locals2 = []
    for k in range(Z):
        columns = slice(k * GENES_Z, (k + 1) * GENES_Z)
        product = jnp.dot(left2, counts_low[:, columns], preferred_element_type=F32)
        gradient = product[:WIDTH]
        weighted = loadings_v[:, columns] * (
            gradient + product[WIDTH : 2 * WIDTH] + product[2 * WIDTH : 3 * WIDTH]
        )
        linear = jnp.where(row < 3, product[3 * WIDTH : 3 * WIDTH + 8], 0.0)
        for n in range(WIDTH // 8):
            linear = linear + weighted[8 * n : 8 * n + 8]
        locals2.append(jnp.concatenate([gradient, bases[k] - linear], axis=0))
    locals2 = swap_blocks(locals2, block)
    for k in range(T):
        local2_out[k] = locals2[k]

    def local2_copy(d):
        target = plane(d)
        return send(
            local2_out.at[target], local2_in.at[t], local2_send.at[d], local2_recv.at[t],
            at(target // YH, z, target % YH, gene),
        )

    def local2_arrived(d):
        source = plane(d)
        slot = local2_in.at[source]
        return send(
            slot, slot, local2_send.at[d], local2_recv.at[source],
            at(source // YH, z, source % YH, gene),
        )

    def local3_copy(d):
        target = (z + d) % Z
        return send(
            local3_out.at[target], local3_in.at[z], local3_send.at[d], local3_recv.at[z],
            at(x, target, yh, gene),
        )

    def local3_arrived(d):
        source = (z + d) % Z
        slot = local3_in.at[source]
        return send(slot, slot, local3_send.at[d], local3_recv.at[source], at(x, source, yh, gene))

    told(6, 9)
    for d in range(1, T):
        local2_copy(d).start()
    local2_in[t] = local2_out[t]

    right2 = right1[:, pl.ds(pl.multiple_of(z * GENES_Z, GENES_Z), GENES_Z)]

    def offsets_of(d):
        logs_z = jnp.log(totals_z[(z + d) % Z].astype(F32)) - LOG_SCALE
        return jnp.concatenate([logs_z[0:1], logs_z[1:2]], axis=1)

    def wait2(first, last):
        for n in range(first, last):
            for side in range(2):
                slot_arrived(ORDER[n], side * 2 + 1 - core).wait_recv()
            totals_arrived(ORDER[n]).wait_recv()

    def expect2(first, last):
        rows = jnp.concatenate([factors_of(ORDER[n]) for n in range(first, last)], axis=1)
        offsets = jnp.concatenate([offsets_of(ORDER[n]) for n in range(first, last)], axis=1)
        columns = slice(first * CELLS, last * CELLS)
        write_table(table2, columns, rows)
        expected = jnp.exp(predict(left_stack(rows, offsets), right2))
        high2[columns, :], low2[columns, :] = two_parts(expected)
        return jnp.sum(expected.reshape((last - first) * CELLS // 8, 8, LANES), axis=0)

    def contract2(first, last, top, bottom):
        columns = slice(first * CELLS, last * CELLS)
        rows = slice(top, bottom)
        main = jnp.dot(table2[rows, columns], high2[columns, :], preferred_element_type=F32)
        sums2[rows, :] = main if first == 0 else sums2[rows, :] + main
        if bottom == ROWS1:
            sums2[TRIANGLE:ROWS1, :] = sums2[TRIANGLE:ROWS1, :] + jnp.dot(
                table2[TRIANGLE:, columns], low2[columns, :], preferred_element_type=F32
            )

    forward(1, 3)
    expected_sum = expect2(0, 1)
    forward(3, 5)
    wait2(1, 3)
    expected_sum = expected_sum + expect2(1, 3)
    forward(5, 7)
    contract2(0, 3, 0, ROWS1)
    forward(7, 8)
    wait2(3, 5)
    expected_sum = expected_sum + expect2(3, 5)
    wait2(5, 7)
    contract2(3, 5, 0, ROWS1)
    expected_sum = expected_sum + expect2(5, 7)
    wait2(7, 8)
    contract2(5, 7, 0, ROWS1)
    expected_sum = expected_sum + expect2(7, 8)
    sums2[ROWS1 : ROWS1 + 8, :] = expected_sum
    sums2[ROWS1 + 8 :, :] = jnp.zeros((ROWS2 - ROWS1 - 8, LANES), F32)

    parts = ((0, 48, piece_out_a, piece_in_a), (T * 48, 40, piece_out_b, piece_in_b))

    def piece_copy(part, d):
        target = plane(d)
        return send(
            parts[part][2].at[target], parts[part][3].at[t],
            piece_send.at[part * T + d], piece_recv.at[part * T + t],
            at(target // YH, z, target % YH, gene),
        )

    def piece_arrived(part, d):
        source = plane(d)
        slot = parts[part][3].at[source]
        return send(
            slot, slot, piece_send.at[part * T + d], piece_recv.at[part * T + source],
            at(source // YH, z, source % YH, gene),
        )

    for part, (top, height, out_ref, in_ref) in enumerate(parts):
        contract2(7, 8, top, min(top + T * height, ROWS1))
        rows = [sums2[top + k * height : top + (k + 1) * height, :] for k in range(T)]
        rows = swap_blocks(rows, block)
        for k in range(T):
            out_ref[k] = rows[k]
        for d in range(1, T):
            piece_copy(part, d).start()
        in_ref[t] = out_ref[t]
    for d in range(1, T):
        local2_arrived(d).wait_recv()
    counts_sum = local2_in[0]
    for k in range(1, T):
        counts_sum = counts_sum + local2_in[k]
    zero = jnp.zeros((8, LANES), F32)
    pieces = [counts_sum[8 * k : 8 * k + 8] for k in range(LOCAL // 8)]
    pieces = swap_blocks(pieces + [zero] * (Z - LOCAL // 8), block)
    for k in range(Z):
        local3_out[k] = pieces[k]
    for d in FAR_FIRST:
        local3_copy(d).start()
    local3_in[z] = local3_out[z]
    for d in ORDER[1:]:
        local3_arrived(d).wait_recv()
    counts_sum = local3_in[0]
    for k in range(1, Z):
        counts_sum = counts_sum + local3_in[k]
    counts_sum = [counts_sum] + [
        pltpu.roll(counts_sum, LANES - k * OWN_GENES, 1) for k in range(1, LOCAL // 8)
    ]
    for part, (top, height, out_ref, in_ref) in enumerate(parts):
        for d in range(1, T):
            piece_arrived(part, d).wait_recv()
        total = in_ref[0]
        for k in range(1, T):
            total = total + in_ref[k]
        for k in range(T):
            packed[top + k * height : top + (k + 1) * height, :] = (
                total if k == 0 else pltpu.roll(total, LANES - k * OWN_GENES, 1)
            )
    load_matrix(matrix, packed)
    old = loadings_v[:, pl.ds(pl.multiple_of(z * GENES_Z, GENES_Z), GENES_Z)]
    own = old
    for k in range(1, T):
        own = jnp.where(t == k, pltpu.roll(old, LANES - k * OWN_GENES, 1), own)
    right[...] = jnp.concatenate(counts_sum[:4], axis=0) - packed[TRIANGLE:ROWS1, :] - RIDGE * own
    new = own + solve(matrix, right, column_a, column_b, inverse)
    mean = jnp.sum(packed[ROWS1 : ROWS1 + 8, :] + counts_sum[4], axis=0, keepdims=True) * (
        2.0 / (CELLS * CELL_DEVICES)
    )

    message = new[:8]
    for k in range(1, 4):
        message = jnp.where(
            block == k, pltpu.roll(new[8 * k : 8 * k + 8], k * OWN_GENES, 1), message
        )
    row = lax.broadcasted_iota(jnp.int32, (8, LANES), 0)
    shifted = pltpu.roll(pltpu.roll(message, HALF, 1), 4, 0)
    message = jnp.where(low, message, shifted)
    final_out[...] = jnp.where(row < 4, message, jnp.broadcast_to(mean, (8, LANES)))

    used = slice(0, MESSAGE)

    places = [(dx, dz, dy) for dx in range(X) for dz in range(Z) for dy in range(YH)]
    places.sort(key=lambda p: -(min(p[0], X - p[0]) + min(p[1], Z - p[1]) + 2 * p[2]))
    places = places[:-1]
    xs = [(x + d) % X for d in range(X)]
    zs = [(z + d) % Z for d in range(Z)]
    ys = [(yh + d) % YH for d in range(YH)]

    def cell_of(place):
        return (xs[place[0]] * Z + zs[place[1]]) * YH + ys[place[2]]

    def final_copy(k):
        return send(
            final_out.at[used], final_hbm.at[t, z, used], final_send.at[k], final_recv.at[cell],
            {"cell": cell_of(places[k]), "gene": gene},
        )

    def final_arrived(k):
        dx, dz, dy = places[k]
        slot = final_hbm.at[xs[dx] * YH + ys[dy], zs[dz], used]
        source = cell_of(places[k])
        return send(
            slot, slot, final_send.at[k], final_recv.at[source], {"cell": source, "gene": gene}
        )

    for k in range(len(places)):
        final_copy(k).start()
    own_final = pltpu.make_async_copy(
        final_out.at[used], final_hbm.at[t, z, used], output_sem.at[1]
    )
    own_final.start()

    for k in range(chunks):
        mirror_copy(k).wait_send()
    for step in range(1, 4):
        local1_copy(step).wait_send()
        near_copy(step).wait_send()
    core_copy.wait_send()
    for d in range(1, Z):
        for side in range(2):
            far_copy(d, side).wait_send()
            forward_copy(d, side).wait_send()
        local3_copy(d).wait_send()
        totals_copy(d).wait_send()
    for d in range(1, T):
        local2_copy(d).wait_send()
        piece_copy(0, d).wait_send()
        piece_copy(1, d).wait_send()
    factors_out.wait()
    own_final.wait()
    for k in range(len(places)):
        final_copy(k).wait_send()
    for k in reversed(range(len(places))):
        final_arrived(k).wait_recv()


def unpack(final_ref, factors_ref, new_factors_ref, new_loadings_ref, deviance_ref):
    new_factors_ref[...] = factors_ref[...]
    lane = lax.broadcasted_iota(jnp.int32, (1, LANES), 1)
    row = lax.broadcasted_iota(jnp.int32, (8 * Z, LANES), 0) % 8
    low = lane < HALF
    slabs = []
    for k in range(T):
        rows = final_ref[k].reshape(8 * Z, LANES)
        turned = pltpu.roll(rows, HALF, 1)
        slabs.append(
            jnp.where(low, jnp.where(row < 4, rows, pltpu.roll(turned, 4, 0)), turned)
        )
    slabs = swap_blocks(slabs, lane // OWN_GENES)
    for k in range(Z):
        eight = slice(8 * k, 8 * k + 8)
        tile = jnp.concatenate([slabs[j][eight] for j in range(4)], axis=0)
        new_loadings_ref[:, k * LANES : (k + 1) * LANES] = tile
        deviance_ref[k : k + 1, :] = slabs[4][8 * k + 4 : 8 * k + 5]


def on_device(counts, totals, cell_factors, gene_loadings):
    hbm, vmem = pl.BlockSpec(memory_space=pltpu.HBM), pl.BlockSpec(memory_space=pltpu.VMEM)
    dma = pltpu.SemaphoreType.DMA
    factors_new, final = pl.pallas_call(
        kernel,
        out_shape=(
            jax.ShapeDtypeStruct((WIDTH, CELLS), F32),
            jax.ShapeDtypeStruct((T, Z, 8, LANES), F32),
        ),
        in_specs=[hbm] * 4,
        out_specs=(hbm,) * 2,
        scratch_shapes=[
            pltpu.VMEM((WIDTH, CELLS), F32),
            pltpu.VMEM((CELLS, GENES), jnp.int32),
            pltpu.VMEM((2, LANES), jnp.int32),
            pltpu.VMEM((Z, 2, LANES), jnp.int32),
            pltpu.VMEM((WIDTH, CELLS), F32),
            pltpu.VMEM((WIDTH, GENES), F32),
            pltpu.VMEM((WIDTH, GENES), F32),
            pltpu.VMEM((6 * WIDTH + 16, GENES), BF16),
            pltpu.VMEM((ROWS1, 2 * GENES), BF16),
            pltpu.VMEM((LANES, 2 * GENES), BF16),
            pltpu.VMEM((LANES, 2 * GENES), BF16),
            pltpu.VMEM((CELLS, GENES), BF16),
            pltpu.VMEM((ROWS1, LANES), F32),
            pltpu.VMEM((4, 16, LANES), F32),
            pltpu.VMEM((4, 16, LANES), F32),
            pltpu.VMEM((ROWS1 // 2, LANES), F32),
            pltpu.VMEM((ROWS1 // 2, LANES), F32),
            pltpu.VMEM((ROWS2, LANES), F32),
            pltpu.VMEM((WIDTH * WIDTH, LANES), F32),
            pltpu.VMEM((WIDTH, LANES), F32),
            pltpu.VMEM((2, WIDTH, LANES), F32),
            pltpu.VMEM((2, WIDTH, LANES), F32),
            pltpu.VMEM((WIDTH + 8, LANES), F32),
            pltpu.VMEM((Z, 4, 16, LANES), F32),
            pltpu.VMEM((T, LOCAL, LANES), F32),
            pltpu.VMEM((T, LOCAL, LANES), F32),
            pltpu.VMEM((Z, 8, LANES), F32),
            pltpu.VMEM((Z, 8, LANES), F32),
            pltpu.VMEM((ROWS1, Z * CELLS), BF16),
            pltpu.VMEM((Z * CELLS, LANES), BF16),
            pltpu.VMEM((Z * CELLS, LANES), BF16),
            pltpu.VMEM((ROWS2, LANES), F32),
            pltpu.VMEM((Z, 8, LANES), F32),
            pltpu.VMEM((T, 48, LANES), F32),
            pltpu.VMEM((T, 48, LANES), F32),
            pltpu.VMEM((T, 40, LANES), F32),
            pltpu.VMEM((T, 40, LANES), F32),
            pltpu.VMEM((8, LANES), F32),
            pltpu.SemaphoreType.REGULAR((9,)),
            dma((4,)), dma((2,)), dma((Z,)), dma((Z,)), dma((8,)), dma((8,)), dma((4,)), dma((4,)),
            dma((1,)), dma((1,)), dma((4 + 2 * Z,)), dma((4 * Z,)), dma((2 * Z,)),
            dma((T,)), dma((T,)), dma((Z,)), dma((Z,)), dma((2 * T,)), dma((2 * T,)),
            dma((CELL_DEVICES,)), dma((CELL_DEVICES,)),
        ],
        compiler_params=pltpu.CompilerParams(
            collective_id=0, has_side_effects=True, vmem_limit_bytes=67043328
        ),
        name="sweep",
    )(counts, totals.reshape(2, LANES), cell_factors.T, gene_loadings.T)
    new_factors, new_loadings, deviance = pl.pallas_call(
        unpack,
        out_shape=(
            jax.ShapeDtypeStruct((WIDTH, CELLS), F32),
            jax.ShapeDtypeStruct((WIDTH, GENES), F32),
            jax.ShapeDtypeStruct((Z, LANES), F32),
        ),
        in_specs=[vmem] * 2,
        out_specs=(vmem,) * 3,
        name="unpack",
    )(final, factors_new)
    return new_factors.T, new_loadings.T, deviance.reshape(GENES)


def solution(mesh):
    return jax.shard_map(
        on_device,
        mesh=mesh,
        in_specs=(P("cell", "gene"), P("cell"), P("cell", None), P("gene", None)),
        out_specs=(P("cell", None), P("gene", None), P("gene")),
        check_vma=False,
    )
```

```python
import math

import jax
import jax.numpy as jnp
from jax import lax
from jax.experimental import pallas as pl
from jax.experimental.pallas import tpu as pltpu
from jax.sharding import PartitionSpec as P

F32, BF16 = jnp.float32, jnp.bfloat16
MESH = pl.DeviceIdType.MESH

RIDGE = 1.0
DAMPING = 0.1
LOG_SCALE = math.log(5000.0)

WIDTH = 32
X, Z, YH = 4, 8, 2
CELL_DEVICES = X * Z * YH
T = X * YH
CELLS = 256
GENES = 1024
LANES = 128
GENES_Z = GENES // Z
OWN_GENES = GENES_Z // T
HALF = LANES // 2
CHUNK = 128
ORDER = (0, 1, 7, 3, 5, 4, 2, 6)
FAR_FIRST = (4, 3, 5, 2, 6, 1, 7)
SENT = (1, 7, 4, 3, 5, 2, 6)
PLANE = ((0, 0), (2, 1), (1, 1), (3, 1), (2, 0), (0, 1), (1, 0), (3, 0))

HEIGHT = [WIDTH - c // 8 * 8 for c in range(WIDTH)]
START = [sum(HEIGHT[:c]) for c in range(WIDTH)]
TRIANGLE = sum(HEIGHT)
ROWS1 = TRIANGLE + WIDTH
LOCAL = WIDTH + 8
ROWS2 = 704
MESSAGE = 5


def parts_of(value):
    high = value.astype(BF16).astype(F32)
    rest = value - high
    middle = rest.astype(BF16).astype(F32)
    return high, middle, rest - middle


def left_stack(factors, offset):
    high, middle, low = parts_of(factors)
    row = lax.broadcasted_iota(jnp.int32, (16, factors.shape[1]), 0)
    off_high, off_middle, off_low = parts_of(offset)
    extra = jnp.where(
        row == 0, off_high, jnp.where(row == 1, off_middle, jnp.where(row == 2, off_low, 0.0))
    )
    return jnp.concatenate([high, high, middle, middle, high, low, extra], axis=0).astype(BF16)


def right_stack(loadings):
    high, middle, low = parts_of(loadings)
    extra = jnp.ones((16, loadings.shape[1]), F32)
    return jnp.concatenate([high, middle, high, middle, low, high, extra], axis=0).astype(BF16)


def predict(left, right):
    return lax.dot_general(left, right, (((0,), (0,)), ((), ())), preferred_element_type=F32)


def write_table(table_ref, columns, rows):
    for c in range(0, WIDTH, 2):
        first = c // 8 * 8
        pair = jnp.concatenate(
            [rows[first:] * rows[c : c + 1], rows[first:] * rows[c + 1 : c + 2]], axis=0
        )
        table_ref[START[c] : START[c] + 2 * HEIGHT[c], columns] = pair.astype(BF16)
    table_ref[TRIANGLE : TRIANGLE + WIDTH, columns] = rows.astype(BF16)


def solve(matrix_ref, right_ref, first_ref, second_ref, inverse_ref):
    for j in range(8, WIDTH):
        for block in range(j // 8):
            matrix_ref[WIDTH * j + 8 * block : WIDTH * j + 8 * block + 8, :] = matrix_ref[
                pl.ds(WIDTH * 8 * block + j, 8, stride=WIDTH), :
            ]
    diagonal = matrix_ref[pl.ds(0, WIDTH, stride=WIDTH + 1), :]
    shift = RIDGE + DAMPING * (jnp.sum(diagonal, axis=0, keepdims=True) / WIDTH)
    matrix_ref[pl.ds(0, WIDTH, stride=WIDTH + 1), :] = diagonal + shift
    row = lax.broadcasted_iota(jnp.int32, (WIDTH, LANES), 0)

    def enter(c, column_ref, first, second):
        column_ref[0] = first
        pivot = 1.0 / column_ref[0, c : c + 1, :]
        inverse_ref[c : c + 1, :] = pivot
        first_scaled = jnp.where(row == c, 0.0, first * pivot)
        second = second - first_scaled * column_ref[0, c + 1 : c + 2, :]
        column_ref[1] = second
        pivot = 1.0 / column_ref[1, c + 1 : c + 2, :]
        inverse_ref[c + 1 : c + 2, :] = pivot
        return first_scaled, jnp.where(row == c + 1, 0.0, second * pivot)

    first, second = enter(0, first_ref, matrix_ref[:WIDTH, :], matrix_ref[WIDTH : 2 * WIDTH, :])
    for c in range(0, WIDTH, 2):
        column_ref, other_ref = (first_ref, second_ref) if c % 4 == 0 else (second_ref, first_ref)

        def reduced(j):
            return (
                matrix_ref[WIDTH * j : WIDTH * j + WIDTH, :]
                - first * column_ref[0, j : j + 1, :]
                - second * column_ref[1, j : j + 1, :]
            )

        if c + 2 < WIDTH:
            after = enter(c + 2, other_ref, reduced(c + 2), reduced(c + 3))
        value = right_ref[...]
        value = value - first * right_ref[c : c + 1, :]
        right_ref[...] = value
        right_ref[...] = value - second * right_ref[c + 1 : c + 2, :]
        for j in range(c + 4, WIDTH):
            matrix_ref[WIDTH * j : WIDTH * j + WIDTH, :] = reduced(j)
        if c + 2 < WIDTH:
            first, second = after
    return right_ref[...] * inverse_ref[:WIDTH, :]


def load_matrix(matrix_ref, packed_ref):
    for c in range(WIDTH):
        first = WIDTH - HEIGHT[c]
        matrix_ref[WIDTH * c + first : WIDTH * c + WIDTH, :] = packed_ref[
            START[c] : START[c] + HEIGHT[c], :
        ]


def swap_blocks(pieces, block):
    pieces = list(pieces)
    for bit in (1, 2, 4):
        keep = (block & bit) == 0
        for k in range(T):
            if k & bit == 0:
                first, second = pieces[k], pieces[k | bit]
                pieces[k] = jnp.where(keep, first, pltpu.roll(second, bit * OWN_GENES, 1))
                pieces[k | bit] = jnp.where(
                    keep, pltpu.roll(first, LANES - bit * OWN_GENES, 1), second
                )
    return pieces


def halves(tile, low):
    middle = tile.shape[0] // 2
    top, bottom = tile[:middle], tile[middle:]
    return (
        jnp.where(low, top, pltpu.roll(bottom, HALF, 1)),
        jnp.where(low, pltpu.roll(top, HALF, 1), bottom),
    )


def two_parts(value):
    high = value.astype(BF16)
    return high, (value - high.astype(F32)).astype(BF16)


def matmul_t(left, right):
    return lax.dot_general(left, right, (((1,), (1,)), ((), ())), preferred_element_type=F32)


def kernel(
    counts_hbm, totals_hbm, factors_hbm, loadings_hbm,
    factors_out_hbm, final_hbm,
    factors_new, counts_v, totals_v, totals_z, factors_v, loadings_v, mirror_v,
    right1, table1, high1, low1, counts_low, sums1, local1_out, local1_in, core_out, core_in,
    packed, matrix, right, column_a, column_b, inverse,
    factor_slots, local2_out, local2_in, local3_out, local3_in, table2, high2, low2, sums2, bases,
    piece_out, piece_in,
    final_out,
    rounds, input_sem, output_sem, totals_send, totals_recv, mirror_send, mirror_recv, local1_send, local1_recv, core_send, core_recv,
    factor_send, factor_recv, forward_send, local2_send, local2_recv, local3_send, local3_recv, piece_send, piece_recv,
    final_send, final_recv,
):
    cell = lax.axis_index("cell")
    gene = lax.axis_index("gene")
    x, z, yh = cell // (Z * YH), (cell // YH) % Z, cell % YH
    yl, core = gene // 2, gene % 2
    t = x * YH + yh
    partner, mirror = yl * 2 + 1 - core, (1 - yl) * 2 + core

    def at(x_, z_, yh_, gene_):
        return {"cell": (x_ * Z + z_) * YH + yh_, "gene": gene_}

    def plane(k):
        return (x + PLANE[k][0]) % X * YH + (yh + PLANE[k][1]) % YH

    def send(src, dst, send_sem, recv_sem, device):
        return pltpu.make_async_remote_copy(
            src_ref=src, dst_ref=dst, send_sem=send_sem, recv_sem=recv_sem,
            device_id=device, device_id_type=MESH,
        )

    def run(action, first, last):
        def body(k, carry):
            action(k)
            return carry

        lax.fori_loop(first, last, body, 0)

    inputs = [
        pltpu.make_async_copy(source, target, input_sem.at[k])
        for k, (source, target) in enumerate(
            [
                (loadings_hbm, loadings_v), (factors_hbm, factors_v),
                (totals_hbm, totals_v), (counts_hbm, counts_v),
            ]
        )
    ]
    for copy in inputs:
        copy.start()

    barrier = pltpu.get_barrier_semaphore()

    def greet(device):
        pl.semaphore_signal(barrier, inc=1, device_id=device, device_id_type=MESH)

    for step in range(1, 4):
        greet(at(x, z, yh, (gene + step) % 4))
    greet(at(x, z, 1 - yh, mirror))
    greet(at(x, z, 1 - yh, gene))
    steps_z, steps_x = (1, Z - 1, 2, Z - 2), (1, X - 1, 2)
    for d in steps_z:
        greet(at(x, (z + d) % Z, yh, gene))
    for d in steps_x:
        greet(at((x + d) % X, z, yh, gene))

    def tell(first, devices):
        for k, device in enumerate(devices):
            pl.semaphore_signal(
                rounds.at[first + k], inc=1, device_id=device, device_id_type=MESH
            )

    def told(first, last):
        for k in range(first, last):
            pl.semaphore_wait(rounds.at[k], 1)

    inputs[0].wait()
    pl.semaphore_wait(barrier, 12)
    tell(0, [at(x, (z + d) % Z, yh, gene) for d in steps_z])
    tell(6, [at((x + d) % X, z, yh, gene) for d in steps_x])

    chunks = GENES // CHUNK

    def mirror_copy(k):
        columns = slice(k * CHUNK, (k + 1) * CHUNK)
        return send(
            loadings_v.at[:, columns], mirror_v.at[:, columns],
            mirror_send.at[k], mirror_recv.at[k],
            at(x, z, yh if k < chunks // 2 else 1 - yh, mirror),
        )

    def totals_copy(d):
        return send(
            totals_v, totals_z.at[z], totals_send.at[d], totals_recv.at[z],
            at(x, (z + d) % Z, yh, gene),
        )

    def totals_arrived(d):
        slot = totals_z.at[(z + d) % Z]
        return send(
            slot, slot, totals_send.at[d], totals_recv.at[(z + d) % Z],
            at(x, (z + d) % Z, yh, gene),
        )

    arrival = [k // 2 + k % 2 * (chunks // 2) for k in range(chunks)]
    for k in arrival:
        mirror_copy(k).start()
    for copy in inputs[1:]:
        copy.wait()

    totals_z[z] = totals_v[...]
    lane = lax.broadcasted_iota(jnp.int32, (1, LANES), 1)
    block = lane // OWN_GENES
    low = lane < HALF
    logs = jnp.log(totals_v[...].astype(F32)) - LOG_SCALE

    lanes_yl = pl.ds(pl.multiple_of(yl * LANES, LANES), LANES)
    old_factors = factors_v[:, lanes_yl]
    left1 = left_stack(old_factors, jnp.where(yl == 0, logs[0:1], logs[1:2]))

    def expect(rows, columns, keep):
        write_table(table1, columns, rows)
        stack = right_stack(rows)
        if keep:
            right1[:, columns] = stack
        high1[:, columns], low1[:, columns] = two_parts(jnp.exp(predict(left1, stack)))

    def contract(columns):
        return (
            matmul_t(table1[:, columns], high1[:, columns]),
            matmul_t(table1[TRIANGLE:, columns], low1[:, columns]),
        )

    for k in range(0, chunks, 2):
        columns = slice(k * CHUNK, (k + 2) * CHUNK)
        expect(loadings_v[:, columns], columns, True)
    main, rest = contract(slice(0, GENES))
    sums1[:TRIANGLE, :] = main[:TRIANGLE]
    sums1[TRIANGLE:, :] = main[TRIANGLE:] + rest

    counts_low[...] = counts_v[...].astype(F32).astype(BF16)
    local1 = matmul_t(table1[TRIANGLE:, :GENES], counts_low[...])
    for pair in range(2):
        packs = halves(local1[:, pair * LANES : (pair + 1) * LANES], low)
        local1_out[2 * pair], local1_out[2 * pair + 1] = packs

    def local1_copy(step):
        target = (gene + step) % 4
        return send(
            local1_out.at[target], local1_in.at[gene],
            local1_send.at[step], local1_recv.at[gene], at(x, z, yh, target),
        )

    def local1_arrived(step):
        source = (gene + step) % 4
        slot = local1_in.at[source]
        return send(
            slot, slot, local1_send.at[step], local1_recv.at[source], at(x, z, yh, source)
        )

    for step in range(1, 4):
        local1_copy(step).start()
    local1_in[gene] = local1_out[gene]

    for k in range(0, chunks, 2):
        for n in range(k, k + 2):
            mirror_copy(arrival[n]).wait_recv()
        rows = jnp.concatenate(
            [mirror_v[:, n * CHUNK : (n + 1) * CHUNK] for n in arrival[k : k + 2]], axis=1
        )
        columns = slice(GENES + k * CHUNK, GENES + (k + 2) * CHUNK)
        expect(rows, columns, False)
        main, rest = contract(columns)
        sums1[:TRIANGLE, :] = sums1[:TRIANGLE, :] + main[:TRIANGLE]
        sums1[TRIANGLE:, :] = sums1[TRIANGLE:, :] + main[TRIANGLE:] + rest

    first_pack, second_pack = halves(sums1[...], low)
    core_out[...] = jnp.where(core == 0, second_pack, first_pack)
    core_copy = send(
        core_out, core_in, core_send.at[0], core_recv.at[0], at(x, z, yh, partner)
    )
    core_copy.start()
    told(0, 4)
    tell(4, [at(x, (z + d) % Z, yh, gene) for d in steps_z[2:]])
    own_pack = jnp.where(core == 0, first_pack, second_pack)
    for step in range(1, 4):
        local1_arrived(step).wait_recv()
    counts_pack = local1_in[0] + local1_in[1] + local1_in[2] + local1_in[3]
    old = jnp.where(core == 0, old_factors, pltpu.roll(old_factors, HALF, 1))
    counts_part = jnp.concatenate([counts_pack, pltpu.roll(counts_pack, HALF, 1)], axis=0)
    core_copy.wait_recv()
    total = own_pack + core_in[...]
    middle = ROWS1 // 2
    packed[:middle, :] = total
    packed[middle:ROWS1, :] = pltpu.roll(total, HALF, 1)
    load_matrix(matrix, packed)
    right[...] = counts_part - packed[TRIANGLE:ROWS1, :] - RIDGE * old
    new = old + solve(matrix, right, column_a, column_b, inverse)
    factor_slots[z, gene] = jnp.where(low, new[:16], pltpu.roll(new[16:], HALF, 1))

    own_slot = factor_slots.at[z, gene]
    own_sem = factor_recv.at[z * 4 + gene]

    def near_copy(step):
        return send(
            own_slot, own_slot, factor_send.at[step], own_sem, at(x, z, yh, (gene + step) % 4)
        )

    def far_copy(d, side):
        return send(
            own_slot, own_slot, factor_send.at[4 + 2 * d + side], own_sem,
            at(x, (z + d) % Z, yh, side * 2 + core),
        )

    def slot_arrived(d, source):
        source_z = (z + d) % Z
        slot = factor_slots.at[source_z, source]
        return send(
            slot, slot, factor_send.at[0], factor_recv.at[source_z * 4 + source],
            at(x, z, yh, partner),
        )

    def forward_copy(d, side):
        source_z, source = (z + d) % Z, side * 2 + core
        slot = factor_slots.at[source_z, source]
        return send(
            slot, slot, forward_send.at[2 * d + side], factor_recv.at[source_z * 4 + source],
            at(x, z, yh, partner),
        )

    for step in range(1, 4):
        near_copy(step).start()
    told(4, 6)
    for d in SENT:
        for side in range(2):
            far_copy(d, side).start()
    for d in SENT:
        totals_copy(d).start()

    def factors_of(d):
        slot = (z + d) % Z
        tiles = []
        for pair in range(2):
            first, second = factor_slots[slot, 2 * pair], factor_slots[slot, 2 * pair + 1]
            tiles.append(
                jnp.concatenate(
                    [
                        jnp.where(low, first, pltpu.roll(second, HALF, 1)),
                        jnp.where(low, pltpu.roll(first, HALF, 1), second),
                    ],
                    axis=0,
                )
            )
        return jnp.concatenate(tiles, axis=1)

    def forward(first, last):
        for n in range(first, last):
            for side in range(2):
                slot_arrived(ORDER[n], side * 2 + core).wait_recv()
                forward_copy(ORDER[n], side).start()

    for k in range(Z):
        counts = counts_v[:, k * GENES_Z : (k + 1) * GENES_Z].astype(F32)
        terms = counts * (jnp.log(jnp.maximum(counts, 1.0)) - 1.0)
        bases[k] = jnp.sum(terms.reshape(CELLS // 8, 8, LANES), axis=0)
    for step in range(1, 4):
        slot_arrived(0, (gene + step) % 4).wait_recv()
    rows = factors_of(0)
    factors_new[...] = rows
    factors_out = pltpu.make_async_copy(factors_new, factors_out_hbm, output_sem.at[0])
    factors_out.start()
    factor_parts = parts_of(rows)
    offset_parts = parts_of(jnp.concatenate([logs[0:1], logs[1:2]], axis=1))
    row = lax.broadcasted_iota(jnp.int32, (16, CELLS), 0)
    extra = jnp.zeros((16, CELLS), F32)
    for k in range(3):
        extra = jnp.where(row == k, offset_parts[k], extra)
    left2 = jnp.concatenate([*factor_parts, extra], axis=0).astype(BF16)
    row = lax.broadcasted_iota(jnp.int32, (8, LANES), 0)
    locals2 = []
    for k in range(Z):
        columns = slice(k * GENES_Z, (k + 1) * GENES_Z)
        product = jnp.dot(left2, counts_low[:, columns], preferred_element_type=F32)
        gradient = product[:WIDTH]
        weighted = loadings_v[:, columns] * (
            gradient + product[WIDTH : 2 * WIDTH] + product[2 * WIDTH : 3 * WIDTH]
        )
        linear = jnp.where(row < 3, product[3 * WIDTH : 3 * WIDTH + 8], 0.0)
        for n in range(WIDTH // 8):
            linear = linear + weighted[8 * n : 8 * n + 8]
        locals2.append(jnp.concatenate([gradient, bases[k] - linear], axis=0))
    locals2 = swap_blocks(locals2, block)
    for k in range(T):
        local2_out[k] = locals2[k]

    def local2_copy(d):
        target = plane(d)
        return send(
            local2_out.at[target], local2_in.at[t], local2_send.at[d], local2_recv.at[t],
            at(target // YH, z, target % YH, gene),
        )

    def local2_arrived(d):
        source = plane(d)
        slot = local2_in.at[source]
        return send(
            slot, slot, local2_send.at[d], local2_recv.at[source],
            at(source // YH, z, source % YH, gene),
        )

    def local3_copy(d):
        target = (z + d) % Z
        return send(
            local3_out.at[target], local3_in.at[z], local3_send.at[d], local3_recv.at[z],
            at(x, target, yh, gene),
        )

    def local3_arrived(d):
        source = (z + d) % Z
        slot = local3_in.at[source]
        return send(slot, slot, local3_send.at[d], local3_recv.at[source], at(x, source, yh, gene))

    told(6, 9)
    for d in range(1, T):
        local2_copy(d).start()
    local2_in[t] = local2_out[t]

    right2 = right1[:, pl.ds(pl.multiple_of(z * GENES_Z, GENES_Z), GENES_Z)]

    def offsets_of(d):
        logs_z = jnp.log(totals_z[(z + d) % Z].astype(F32)) - LOG_SCALE
        return jnp.concatenate([logs_z[0:1], logs_z[1:2]], axis=1)

    def wait2(first, last):
        for n in range(first, last):
            for side in range(2):
                slot_arrived(ORDER[n], side * 2 + 1 - core).wait_recv()
            totals_arrived(ORDER[n]).wait_recv()

    def expect2(first, last):
        rows = jnp.concatenate([factors_of(ORDER[n]) for n in range(first, last)], axis=1)
        offsets = jnp.concatenate([offsets_of(ORDER[n]) for n in range(first, last)], axis=1)
        columns = slice(first * CELLS, last * CELLS)
        write_table(table2, columns, rows)
        expected = jnp.exp(predict(left_stack(rows, offsets), right2))
        high2[columns, :], low2[columns, :] = two_parts(expected)
        return jnp.sum(expected.reshape((last - first) * CELLS // 8, 8, LANES), axis=0)

    def contract2(first, last, top, bottom):
        columns = slice(first * CELLS, last * CELLS)
        rows = slice(top, bottom)
        main = jnp.dot(table2[rows, columns], high2[columns, :], preferred_element_type=F32)
        sums2[rows, :] = main if first == 0 else sums2[rows, :] + main
        if bottom == ROWS1:
            sums2[TRIANGLE:ROWS1, :] = sums2[TRIANGLE:ROWS1, :] + jnp.dot(
                table2[TRIANGLE:, columns], low2[columns, :], preferred_element_type=F32
            )

    forward(1, 3)
    expected_sum = expect2(0, 1)
    forward(3, 5)
    wait2(1, 3)
    expected_sum = expected_sum + expect2(1, 3)
    forward(5, 7)
    contract2(0, 3, 0, ROWS1)
    forward(7, 8)
    wait2(3, 5)
    expected_sum = expected_sum + expect2(3, 5)
    wait2(5, 7)
    contract2(3, 5, 0, ROWS1)
    expected_sum = expected_sum + expect2(5, 7)
    wait2(7, 8)
    contract2(5, 7, 0, ROWS1)
    expected_sum = expected_sum + expect2(7, 8)
    sums2[ROWS1 : ROWS1 + 8, :] = expected_sum
    sums2[ROWS1 + 8 :, :] = jnp.zeros((ROWS2 - ROWS1 - 8, LANES), F32)

    parts = ((0, ROWS2 // T, piece_out, piece_in),)

    def piece_copy(part, d):
        target = plane(d)
        return send(
            parts[part][2].at[target], parts[part][3].at[t],
            piece_send.at[part * T + d], piece_recv.at[part * T + t],
            at(target // YH, z, target % YH, gene),
        )

    def piece_arrived(part, d):
        source = plane(d)
        slot = parts[part][3].at[source]
        return send(
            slot, slot, piece_send.at[part * T + d], piece_recv.at[part * T + source],
            at(source // YH, z, source % YH, gene),
        )

    for part, (top, height, out_ref, in_ref) in enumerate(parts):
        contract2(7, 8, top, min(top + T * height, ROWS1))
        rows = [sums2[top + k * height : top + (k + 1) * height, :] for k in range(T)]
        rows = swap_blocks(rows, block)
        for k in range(T):
            out_ref[k] = rows[k]
        for d in range(1, T):
            piece_copy(part, d).start()
        in_ref[t] = out_ref[t]
    for d in range(1, T):
        local2_arrived(d).wait_recv()
    counts_sum = local2_in[0]
    for k in range(1, T):
        counts_sum = counts_sum + local2_in[k]
    zero = jnp.zeros((8, LANES), F32)
    pieces = [counts_sum[8 * k : 8 * k + 8] for k in range(LOCAL // 8)]
    pieces = swap_blocks(pieces + [zero] * (Z - LOCAL // 8), block)
    for k in range(Z):
        local3_out[k] = pieces[k]
    for d in FAR_FIRST:
        local3_copy(d).start()
    local3_in[z] = local3_out[z]
    for d in ORDER[1:]:
        local3_arrived(d).wait_recv()
    counts_sum = local3_in[0]
    for k in range(1, Z):
        counts_sum = counts_sum + local3_in[k]
    counts_sum = [counts_sum] + [
        pltpu.roll(counts_sum, LANES - k * OWN_GENES, 1) for k in range(1, LOCAL // 8)
    ]
    for part, (top, height, out_ref, in_ref) in enumerate(parts):
        for d in range(1, T):
            piece_arrived(part, d).wait_recv()
        total = in_ref[0]
        for k in range(1, T):
            total = total + in_ref[k]
        for k in range(T):
            packed[top + k * height : top + (k + 1) * height, :] = (
                total if k == 0 else pltpu.roll(total, LANES - k * OWN_GENES, 1)
            )
    load_matrix(matrix, packed)
    old = loadings_v[:, pl.ds(pl.multiple_of(z * GENES_Z, GENES_Z), GENES_Z)]
    own = old
    for k in range(1, T):
        own = jnp.where(t == k, pltpu.roll(old, LANES - k * OWN_GENES, 1), own)
    right[...] = jnp.concatenate(counts_sum[:4], axis=0) - packed[TRIANGLE:ROWS1, :] - RIDGE * own
    new = own + solve(matrix, right, column_a, column_b, inverse)
    mean = jnp.sum(packed[ROWS1 : ROWS1 + 8, :] + counts_sum[4], axis=0, keepdims=True) * (
        2.0 / (CELLS * CELL_DEVICES)
    )

    message = new[:8]
    for k in range(1, 4):
        message = jnp.where(
            block == k, pltpu.roll(new[8 * k : 8 * k + 8], k * OWN_GENES, 1), message
        )
    row = lax.broadcasted_iota(jnp.int32, (8, LANES), 0)
    shifted = pltpu.roll(pltpu.roll(message, HALF, 1), 4, 0)
    message = jnp.where(low, message, shifted)
    final_out[...] = jnp.where(row < 4, message, jnp.broadcast_to(mean, (8, LANES)))

    used = slice(0, MESSAGE)

    places = [(dx, dz, dy) for dx in range(X) for dz in range(Z) for dy in range(YH)]
    places.sort(key=lambda p: -(min(p[0], X - p[0]) + min(p[1], Z - p[1]) + 2 * p[2]))
    places = places[:-1]
    xs = [(x + d) % X for d in range(X)]
    zs = [(z + d) % Z for d in range(Z)]
    ys = [(yh + d) % YH for d in range(YH)]

    def cell_of(place):
        return (xs[place[0]] * Z + zs[place[1]]) * YH + ys[place[2]]

    def final_copy(k):
        return send(
            final_out.at[used], final_hbm.at[t, z, used], final_send.at[k], final_recv.at[cell],
            {"cell": cell_of(places[k]), "gene": gene},
        )

    def final_arrived(k):
        dx, dz, dy = places[k]
        slot = final_hbm.at[xs[dx] * YH + ys[dy], zs[dz], used]
        source = cell_of(places[k])
        return send(
            slot, slot, final_send.at[k], final_recv.at[source], {"cell": source, "gene": gene}
        )

    for k in range(len(places)):
        final_copy(k).start()
    own_final = pltpu.make_async_copy(
        final_out.at[used], final_hbm.at[t, z, used], output_sem.at[1]
    )
    own_final.start()

    for k in range(chunks):
        mirror_copy(k).wait_send()
    for step in range(1, 4):
        local1_copy(step).wait_send()
        near_copy(step).wait_send()
    core_copy.wait_send()
    for d in range(1, Z):
        for side in range(2):
            far_copy(d, side).wait_send()
            forward_copy(d, side).wait_send()
        local3_copy(d).wait_send()
        totals_copy(d).wait_send()
    for d in range(1, T):
        local2_copy(d).wait_send()
        piece_copy(0, d).wait_send()
    factors_out.wait()
    own_final.wait()
    for k in range(len(places)):
        final_copy(k).wait_send()
    for k in reversed(range(len(places))):
        final_arrived(k).wait_recv()


def unpack(final_ref, factors_ref, new_factors_ref, new_loadings_ref, deviance_ref):
    new_factors_ref[...] = factors_ref[...]
    lane = lax.broadcasted_iota(jnp.int32, (1, LANES), 1)
    row = lax.broadcasted_iota(jnp.int32, (8 * Z, LANES), 0) % 8
    low = lane < HALF
    slabs = []
    for k in range(T):
        rows = final_ref[k].reshape(8 * Z, LANES)
        turned = pltpu.roll(rows, HALF, 1)
        slabs.append(
            jnp.where(low, jnp.where(row < 4, rows, pltpu.roll(turned, 4, 0)), turned)
        )
    slabs = swap_blocks(slabs, lane // OWN_GENES)
    for k in range(Z):
        eight = slice(8 * k, 8 * k + 8)
        tile = jnp.concatenate([slabs[j][eight] for j in range(4)], axis=0)
        new_loadings_ref[:, k * LANES : (k + 1) * LANES] = tile
        deviance_ref[k : k + 1, :] = slabs[4][8 * k + 4 : 8 * k + 5]


def on_device(counts, totals, cell_factors, gene_loadings):
    hbm, vmem = pl.BlockSpec(memory_space=pltpu.HBM), pl.BlockSpec(memory_space=pltpu.VMEM)
    dma = pltpu.SemaphoreType.DMA
    factors_new, final = pl.pallas_call(
        kernel,
        out_shape=(
            jax.ShapeDtypeStruct((WIDTH, CELLS), F32),
            jax.ShapeDtypeStruct((T, Z, 8, LANES), F32),
        ),
        in_specs=[hbm] * 4,
        out_specs=(hbm,) * 2,
        scratch_shapes=[
            pltpu.VMEM((WIDTH, CELLS), F32),
            pltpu.VMEM((CELLS, GENES), jnp.int32),
            pltpu.VMEM((2, LANES), jnp.int32),
            pltpu.VMEM((Z, 2, LANES), jnp.int32),
            pltpu.VMEM((WIDTH, CELLS), F32),
            pltpu.VMEM((WIDTH, GENES), F32),
            pltpu.VMEM((WIDTH, GENES), F32),
            pltpu.VMEM((6 * WIDTH + 16, GENES), BF16),
            pltpu.VMEM((ROWS1, 2 * GENES), BF16),
            pltpu.VMEM((LANES, 2 * GENES), BF16),
            pltpu.VMEM((LANES, 2 * GENES), BF16),
            pltpu.VMEM((CELLS, GENES), BF16),
            pltpu.VMEM((ROWS1, LANES), F32),
            pltpu.VMEM((4, 16, LANES), F32),
            pltpu.VMEM((4, 16, LANES), F32),
            pltpu.VMEM((ROWS1 // 2, LANES), F32),
            pltpu.VMEM((ROWS1 // 2, LANES), F32),
            pltpu.VMEM((ROWS2, LANES), F32),
            pltpu.VMEM((WIDTH * WIDTH, LANES), F32),
            pltpu.VMEM((WIDTH, LANES), F32),
            pltpu.VMEM((2, WIDTH, LANES), F32),
            pltpu.VMEM((2, WIDTH, LANES), F32),
            pltpu.VMEM((WIDTH + 8, LANES), F32),
            pltpu.VMEM((Z, 4, 16, LANES), F32),
            pltpu.VMEM((T, LOCAL, LANES), F32),
            pltpu.VMEM((T, LOCAL, LANES), F32),
            pltpu.VMEM((Z, 8, LANES), F32),
            pltpu.VMEM((Z, 8, LANES), F32),
            pltpu.VMEM((ROWS1, Z * CELLS), BF16),
            pltpu.VMEM((Z * CELLS, LANES), BF16),
            pltpu.VMEM((Z * CELLS, LANES), BF16),
            pltpu.VMEM((ROWS2, LANES), F32),
            pltpu.VMEM((Z, 8, LANES), F32),
            pltpu.VMEM((T, ROWS2 // T, LANES), F32),
            pltpu.VMEM((T, ROWS2 // T, LANES), F32),
            pltpu.VMEM((8, LANES), F32),
            pltpu.SemaphoreType.REGULAR((9,)),
            dma((4,)), dma((2,)), dma((Z,)), dma((Z,)), dma((8,)), dma((8,)), dma((4,)), dma((4,)),
            dma((1,)), dma((1,)), dma((4 + 2 * Z,)), dma((4 * Z,)), dma((2 * Z,)),
            dma((T,)), dma((T,)), dma((Z,)), dma((Z,)), dma((2 * T,)), dma((2 * T,)),
            dma((CELL_DEVICES,)), dma((CELL_DEVICES,)),
        ],
        compiler_params=pltpu.CompilerParams(
            collective_id=0, has_side_effects=True, vmem_limit_bytes=67043328
        ),
        name="sweep",
    )(counts, totals.reshape(2, LANES), cell_factors.T, gene_loadings.T)
    new_factors, new_loadings, deviance = pl.pallas_call(
        unpack,
        out_shape=(
            jax.ShapeDtypeStruct((WIDTH, CELLS), F32),
            jax.ShapeDtypeStruct((WIDTH, GENES), F32),
            jax.ShapeDtypeStruct((Z, LANES), F32),
        ),
        in_specs=[vmem] * 2,
        out_specs=(vmem,) * 3,
        name="unpack",
    )(final, factors_new)
    return new_factors.T, new_loadings.T, deviance.reshape(GENES)


def solution(mesh):
    return jax.shard_map(
        on_device,
        mesh=mesh,
        in_specs=(P("cell", "gene"), P("cell"), P("cell", None), P("gene", None)),
        out_specs=(P("cell", None), P("gene", None), P("gene")),
        check_vma=False,
    )
```
